32 devices in a mesh: fsdp: 4 (over y, x), tp: 8 (over z, core).
Axes of the slice: x: 2, y: 2, z: 4, core: 2. Of those that a mesh axis runs over, the one named last changes fastest.
Arguments:
- inputs: bfloat16 [2, 4, 2048, 2048], P(None, 'fsdp', 'tp'), may hold values from -6 to 6
- out_grad: bfloat16 [2, 4, 2048, 2048], P(None, 'fsdp', 'tp'), may hold values from -6 to 6
- lengths: int32 [2, 4], replicated, may hold values from 1024 to 2048, as said below
- norm1_gain: bfloat16 [2048], P('fsdp'), may hold values from 0.099609375 to 1.8984375
- qkv_weight: bfloat16 [2048, 3, 2048], P('fsdp', None, 'tp'), may hold values from -0.125 to 0.125
- out_weight: bfloat16 [2048, 2048], P('tp', 'fsdp'), may hold values from -0.75 to 0.75
- norm2_gain: bfloat16 [2048], P('fsdp'), may hold values from 0.099609375 to 1.8984375
- gate_up_weight: bfloat16 [2048, 2, 8192], P('fsdp', None, 'tp'), may hold values from -0.125 to 0.125
- down_weight: bfloat16 [8192, 2048], P('tp', 'fsdp'), may hold values from -0.0625 to 0.0625
Outputs:
- outputs: bfloat16 [2, 4, 2048, 2048], P(None, 'fsdp', 'tp')
- input_grad: bfloat16 [2, 4, 2048, 2048], P(None, 'fsdp', 'tp')
- norm1_gain_grad: float32 [2048], P('fsdp')
- qkv_grad: float32 [2048, 3, 2048], P('fsdp', None, 'tp')
- out_weight_grad: float32 [2048, 2048], P('tp', 'fsdp')
- norm2_gain_grad: float32 [2048], P('fsdp')
- gate_up_grad: float32 [2048, 2, 8192], P('fsdp', None, 'tp')
- down_grad: float32 [8192, 2048], P('tp', 'fsdp')
The draws below stay inside these ranges and needn't reach their ends.
Inputs may be any that keep to these rules, and one draw needn't show every extreme that they name: lengths[m, g] tokens of the sequence of micro-batch m and group g are live, at its start; where m + g is even there are more than 1536 of them, else fewer than 1536.
All inputs are finite; a program needn't handle non-finite values.
Results may differ from the reference program's by a relative error of at most 0.024.
Values may be sent and summed in bfloat16 or wider, within the bound.
A program may use at most 184 MiB of HBM per device.

```python
import math
import jax
import jax.numpy as jnp
from jax import lax

D = 2048
H = 32
HD = 64
FF = 8192
SEQ = 2048
MB = 2
SEQS = 4


def draw_lengths(key, part):
    micro_rows = jnp.arange(MB)[:, None]
    group_cols = jnp.arange(SEQS)[None, :]
    offset = jax.random.randint(key, (MB, SEQS), 0, SEQ // 4)
    leading = jnp.logical_and(micro_rows == 0, group_cols < 2)
    offset = jnp.where(leading, 0, offset)
    longer = (micro_rows + group_cols) % 2 == 0
    return jnp.where(longer, SEQ - offset, SEQ // 2 + offset).astype(jnp.int32)


def shard_levels(stream_key, shape, pieces, smallest, top_value):
    level, own = 1.0, jax.random.fold_in(stream_key, 6)
    for dim, shards_of in pieces:
        steps = jnp.exp(jax.random.uniform(jax.random.fold_in(own, dim), (shards_of,), jnp.float32, smallest / len(pieces), top_value / len(pieces)))
        level = level * jnp.repeat(steps, shape[dim] // shards_of).reshape([-1 if axis == dim else 1 for axis in range(len(shape))])
    return level


def scatter_about(key, shape, spread, most, pieces=(), kind=jnp.bfloat16):
    drawn = jax.random.normal(key, shape, jnp.float32) * spread
    if len(pieces) > 0:
        drawn = shard_levels(key, shape, pieces, -0.22, 0.18) * drawn
    return jnp.clip(drawn, min=-most, max=most).astype(kind)


def setup_inputs(seed: int = 0) -> dict:
    key_list = jax.random.split(jax.random.key(seed), 10)
    inputs = scatter_about(key_list[0], (MB, SEQS, SEQ, D), 1.0, 6.0, ((1, 4), (2, 8)))
    out_grad = scatter_about(key_list[1], (MB, SEQS, SEQ, D), 1.0, 6.0, ((1, 4), (2, 8)))
    lengths = draw_lengths(jax.random.fold_in(key_list[9], 71), 0)
    norm1_gain = jnp.clip(1.0 + 0.18 * jax.random.normal(key_list[3], (D,), jnp.float32), 0.099609375, 1.8984375).astype(jnp.bfloat16)
    qkv_weight = scatter_about(key_list[4], (D, 3, D), D ** -0.5, 0.125, ((0, 4), (2, 8)))
    out_weight = scatter_about(key_list[5], (D, D), (D // 32) ** -0.5, 0.75, ((0, 8), (1, 4)))
    norm2_gain = jnp.clip(1.0 + 0.18 * jax.random.normal(key_list[6], (D,), jnp.float32), 0.099609375, 1.8984375).astype(jnp.bfloat16)
    gate_up_weight = scatter_about(key_list[7], (D, 2, FF), D ** -0.5, 0.125, ((0, 4), (2, 8)))
    down_weight = scatter_about(key_list[8], (FF, D), FF ** -0.5, 0.0625, ((0, 8), (1, 4)))
    return dict(inputs=inputs, out_grad=out_grad, lengths=lengths, norm1_gain=norm1_gain, qkv_weight=qkv_weight, out_weight=out_weight, norm2_gain=norm2_gain, gate_up_weight=gate_up_weight, down_weight=down_weight)


@jax.custom_vjp
def low(v):
    return lax.optimization_barrier(v.astype(jnp.bfloat16)).astype(jnp.float32)

@jax.custom_vjp
def low_back(v):
    return v

def low_keep(v):
    return (low(v), None)

def low_pass(kept, grad):
    return (grad,)

def back_keep(v):
    return (v, None)

def back_low(kept, grad):
    return (low(grad),)
low.defvjp(low_keep, low_pass)
low_back.defvjp(back_keep, back_low)
NORM_EPS = 1e-05
ROPE_THETA = 130000.0
MASKED = -1e+30
FULL_PRECISION = lax.Precision.HIGHEST

def matmul(left_op, right_op):
    return jnp.dot(left_op, right_op, precision=FULL_PRECISION, preferred_element_type=jnp.float32)

def rms_scale(residual, gain_vec):
    factor = lax.rsqrt(lax.optimization_barrier(jnp.mean(residual * residual, axis=-1, keepdims=True)) + NORM_EPS)
    return residual * factor * gain_vec

def rope_tables(seq_len):
    positions = jnp.arange(seq_len).astype(jnp.float32)
    inverse = ROPE_THETA ** (-(jnp.arange(HD // 2).astype(jnp.float32) * 2.0) / HD)
    angles = positions[:, None] * inverse[None, :]
    angles = jnp.concatenate([angles, angles], axis=-1)
    return (jnp.cos(angles), jnp.sin(angles))

def rotate(vectors, cos_tab, sin_tab):
    half_dim = vectors.shape[-1] // 2
    turned = jnp.concatenate([-vectors[..., half_dim:], vectors[..., :half_dim]], axis=-1)
    return vectors * cos_tab[:, None, :] + turned * sin_tab[:, None, :]

def attention(queries, key_heads, value_heads, length):
    seq_len = queries.shape[0]
    block_rows = min(512, seq_len)
    count_blocks = seq_len // block_rows
    key_pos = jnp.arange(seq_len)
    score_scale = 1.0 / math.sqrt(HD)

    def query_block(element):
        q_block, begin_row = element
        scores = jnp.einsum('qhe,khe->hqk', q_block, key_heads, precision=FULL_PRECISION, preferred_element_type=jnp.float32) * score_scale
        scores = low_back(scores)
        query_pos = begin_row + jnp.arange(block_rows)
        allowed = (key_pos[None, :] <= query_pos[:, None]) & (key_pos[None, :] < length)
        scores = jnp.where(allowed[None], scores, MASKED)
        top_score = lax.optimization_barrier(jnp.max(scores, axis=-1, keepdims=True))
        exponent = jnp.exp(scores - top_score)
        attn_probs = low(exponent / lax.optimization_barrier(jnp.sum(exponent, axis=-1, keepdims=True)))
        return jnp.einsum('hqk,khe->qhe', attn_probs, value_heads, precision=FULL_PRECISION, preferred_element_type=jnp.float32)
    blocked = queries.reshape(count_blocks, block_rows, queries.shape[1], queries.shape[2])
    begins = (jnp.arange(count_blocks) * block_rows).astype(jnp.int32)
    outputs = lax.map(jax.checkpoint(query_block), (blocked, begins))
    return outputs.reshape(seq_len, -1)

def layer_forward(residual, length, gain_one, qkv_w, out_w, gain_two, gate_up_w, down_w):
    seq_len = residual.shape[0]
    cos_tab, sin_tab = rope_tables(seq_len)
    normed = low(rms_scale(residual, gain_one))
    raw_proj = low_back(matmul(normed, qkv_w.reshape(D, 3 * D))).reshape(seq_len, 3, H, HD)
    queries = low(rotate(raw_proj[:, 0], cos_tab, sin_tab))
    key_heads = low(rotate(raw_proj[:, 1], cos_tab, sin_tab))
    value_heads = low(raw_proj[:, 2])
    attn_mixed = low(low_back(attention(queries, key_heads, value_heads, length)))
    middle = residual + low_back(matmul(attn_mixed, out_w))
    normed_two = low(rms_scale(middle, gain_two))
    gate_up = low_back(matmul(normed_two, gate_up_w.reshape(D, 2 * FF)))
    hidden = low(jax.nn.silu(gate_up[:, :FF]) * gate_up[:, FF:])
    result = middle + low_back(matmul(hidden, down_w))
    live_rows = (jnp.arange(seq_len) < length).astype(residual.dtype)
    return result * live_rows[:, None]

def reference(inputs, out_grad, lengths, norm1_gain, qkv_weight, out_weight, norm2_gain, gate_up_weight, down_weight):
    weights = (norm1_gain.astype(jnp.float32), qkv_weight.astype(jnp.float32), out_weight.astype(jnp.float32), norm2_gain.astype(jnp.float32), gate_up_weight.astype(jnp.float32), down_weight.astype(jnp.float32))
    flat_in = inputs.astype(jnp.float32).reshape(MB * SEQS, SEQ, D)
    flat_grad = out_grad.astype(jnp.float32).reshape(MB * SEQS, SEQ, D)
    flat_len = lengths.reshape(MB * SEQS)

    def seq_step(totals, element):
        residual, cotangent, length = element

        def forward_fn(resid_in, *params):
            return layer_forward(resid_in, length, *params)
        result, pullback = jax.vjp(forward_fn, residual, *weights)
        gradients = pullback(cotangent)
        totals = tuple((total + grad_w for total, grad_w in zip(totals, gradients[1:])))
        return (totals, (result.astype(jnp.bfloat16), gradients[0].astype(jnp.bfloat16)))
    start_totals = tuple((jnp.zeros(weight_arr.shape, jnp.float32) for weight_arr in weights))
    totals, (outputs, input_grads) = lax.scan(seq_step, start_totals, (flat_in, flat_grad, flat_len))
    shape_out = (MB, SEQS, SEQ, D)
    return (outputs.reshape(shape_out), input_grads.reshape(shape_out), totals[0], totals[1], totals[2], totals[3], totals[4], totals[5])
```

```python
import functools
import math

import jax
import jax.numpy as jnp
from jax import lax
from jax.experimental import pallas as pl
from jax.experimental.pallas import tpu as pltpu
from jax.sharding import Mesh
from jax.sharding import PartitionSpec as P

HD = 64
NORM_EPS = 1e-05
ROPE_THETA = 130000.0
BLK = 256
SEG = 2
BF = jnp.bfloat16
F32 = jnp.float32
NEG = -1e30
SCALE = 1.0 / math.sqrt(HD)
LOG2E = math.log2(math.e)
VMEM_BYTES = 60 * 1024 * 1024


def swap(x, axis, bit):
    size = lax.axis_size(axis)
    return lax.ppermute(x, axis, [(i, i ^ bit) for i in range(size)])


def gather_slots(x, axis):
    size = lax.axis_size(axis)
    slots = {0: x}
    bit = size // 2
    while bit:
        for k in list(slots):
            slots[k | bit] = swap(slots[k], axis, bit)
        bit //= 2
    return [slots[k] for k in range(size)]


def scatter_slots(parts, axis):
    slots = dict(enumerate(parts))
    bit = 1
    while bit < lax.axis_size(axis):
        for k in [k for k in slots if k & bit]:
            got = swap(slots.pop(k), axis, bit)
            kept = slots[k ^ bit].astype(F32) + got.astype(F32)
            slots[k ^ bit] = kept if bit * 2 == lax.axis_size(axis) else kept.astype(BF)
        bit *= 2
    return slots[0]


def gather_rows(local):
    halves, rows, dim = local.shape
    blocks = gather_slots(local, "tp")
    return jnp.stack(blocks, axis=1).reshape(halves * len(blocks) * rows, dim)


def scatter_rows(full, rows):
    size = lax.axis_size("tp")
    parts = full.reshape(2, size, rows, full.shape[-1])
    return scatter_slots([parts[:, k] for k in range(size)], "tp")


def qkv_kernel(x_ref, w_ref, cos_ref, sa_ref, sb_ref, o_ref):
    acc = jnp.dot(x_ref[...], w_ref[...], preferred_element_type=F32)
    cos, sin_a, sin_b = cos_ref[...], sa_ref[...], sb_ref[...]
    for part in range(o_ref.shape[1] // 128):
        lanes = slice(part * 128, part * 128 + 128)
        u = acc[:, lanes]
        if part % 3 < 2:
            u = u * cos + pltpu.roll(u, 96, 1) * sin_a + pltpu.roll(u, 32, 1) * sin_b
        o_ref[:, lanes] = u.astype(BF)


def qkv_project(rows, weight, cos, sin_a, sin_b):
    seq, dim = rows.shape
    cols = weight.shape[1]
    row_block = min(BLK, seq)
    return pl.pallas_call(
        qkv_kernel,
        grid=(seq // row_block,),
        in_specs=[
            pl.BlockSpec((row_block, dim), lambda i: (i, 0)),
            pl.BlockSpec((dim, cols), lambda i: (0, 0), pipeline_mode=pl.Buffered(1)),
        ]
        + [pl.BlockSpec((row_block, 128), lambda i: (i, 0))] * 3,
        out_specs=pl.BlockSpec((row_block, cols), lambda i: (i, 0)),
        out_shape=jax.ShapeDtypeStruct((seq, cols), BF),
        compiler_params=pltpu.CompilerParams(vmem_limit_bytes=VMEM_BYTES),
        cost_estimate=pl.CostEstimate(
            flops=2 * seq * dim * cols, bytes_accessed=2 * (seq * dim + dim * cols + seq * cols), transcendentals=0
        ),
        name="qkv_project",
    )(rows, weight, cos, sin_a, sin_b)


def slot_of(block, group, turn):
    return (block // group) * group + jnp.bitwise_xor(block % group, turn)


def lane_masks(rows):
    lane = lax.broadcasted_iota(jnp.int32, (rows, 128), 1)
    return lane < HD, lane >= HD


def diagonal_mask(block, length):
    key = lax.broadcasted_iota(jnp.int32, (BLK, BLK), 0)
    query = lax.broadcasted_iota(jnp.int32, (BLK, BLK), 1)
    return (key <= query) & (key + block * BLK < length)


def attend_kernel(group, info_ref, qkv_ref, o_ref, lse_ref, vt_ref):
    count = qkv_ref.shape[0] // BLK
    length, turn = info_ref[0], info_ref[1]

    def rows_of(block):
        return pl.ds(pl.multiple_of(slot_of(block, group, turn) * BLK, BLK), BLK)

    masks = lane_masks(BLK)
    for i in range(count):

        @pl.when(i * BLK < length)
        def _():
            where_q = rows_of(i)
            vt_ref[i] = qkv_ref[where_q, 256:384].T
            q = qkv_ref[where_q, 0:128]
            outs = []
            for h in range(2):
                qt = jnp.where(masks[h], q, jnp.zeros_like(q)).T
                top = total = acc = None
                step = 2
                first = 0
                while first <= i:
                    blocks = list(range(first, min(first + step, i + 1)))
                    scores = []
                    for b in blocks:
                        s = jnp.dot(qkv_ref[rows_of(b), 128:256], qt, preferred_element_type=F32) * (SCALE * LOG2E)
                        if b == i:
                            s = jnp.where(diagonal_mask(i, length), s, NEG)
                        scores.append(s)
                    new_top = functools.reduce(jnp.maximum, [jnp.max(s, axis=0, keepdims=True) for s in scores])
                    if top is not None:
                        new_top = jnp.maximum(top, new_top)
                        fade = jnp.exp2(top - new_top)
                        total, acc = total * fade, acc * fade
                    for b, s in zip(blocks, scores):
                        p = jnp.exp2(s - new_top)
                        p_sum = jnp.sum(p, axis=0, keepdims=True)
                        mixed = jnp.dot(
                            vt_ref[b, h * HD : h * HD + HD, :], p.astype(BF), preferred_element_type=F32
                        )
                        total = p_sum if total is None else total + p_sum
                        acc = mixed if acc is None else acc + mixed
                    top = new_top
                    first += step
                outs.append(acc / total)
                lse_ref[i, h : h + 1, :] = top + jnp.log2(total)
            o_ref[where_q, :] = jnp.concatenate(outs, axis=0).T.astype(BF)

        @pl.when(i * BLK >= length)
        def _():
            o_ref[rows_of(i), :] = jnp.zeros((BLK, 128), BF)
            lse_ref[i] = jnp.zeros((2, BLK), F32)


def attend(info, qkv, group):
    seq, cols = qkv.shape
    pairs = cols // 384
    count = seq // BLK
    return pl.pallas_call(
        functools.partial(attend_kernel, group),
        grid_spec=pltpu.PrefetchScalarGridSpec(
            num_scalar_prefetch=1,
            grid=(pairs,),
            in_specs=[pl.BlockSpec((seq, 384), lambda p, s: (0, p))],
            out_specs=[
                pl.BlockSpec((seq, 128), lambda p, s: (0, p)),
                pl.BlockSpec((None, count, 2, BLK), lambda p, s: (p, 0, 0, 0)),
            ],
            scratch_shapes=[pltpu.VMEM((count, 128, BLK), BF)],
        ),
        out_shape=[
            jax.ShapeDtypeStruct((seq, pairs * 128), BF),
            jax.ShapeDtypeStruct((pairs, count, 2, BLK), F32),
        ],
        compiler_params=pltpu.CompilerParams(vmem_limit_bytes=VMEM_BYTES),
        cost_estimate=pl.CostEstimate(
            flops=pairs * 2 * seq * seq * 2 * 256, bytes_accessed=2 * seq * pairs * 512, transcendentals=pairs * seq * seq
        ),
        name="attend",
    )(info, qkv)


def rope_back(w, cos_t, sin_t):
    half = HD // 2
    upper, lower = w[:half], w[half:]
    return jnp.concatenate([upper * cos_t + lower * sin_t, lower * cos_t - upper * sin_t], axis=0)


def attend_back_kernel(
    group, info_ref, qkv_ref, o_ref, do_ref, lse_ref, cos_ref, sin_ref, d_ref, kt_ref, dk_ref, dv_ref
):
    count = qkv_ref.shape[0] // BLK
    length, turn = info_ref[0], info_ref[1]

    def rows_of(block):
        return pl.ds(pl.multiple_of(slot_of(block, group, turn) * BLK, BLK), BLK)

    masks = lane_masks(BLK)
    for i in range(count):

        @pl.when(i * BLK < length)
        def _():
            where_q = rows_of(i)
            kt_ref[i] = qkv_ref[where_q, 128:256].T
            q = qkv_ref[where_q, 0:128]
            do = do_ref[where_q, :]
            product = (o_ref[where_q, :].astype(F32) * do.astype(F32)).T
            zero = jnp.zeros_like(q)
            dq_t = []
            for h in range(2):
                q_h = jnp.where(masks[h], q, zero)
                do_h = jnp.where(masks[h], do, zero)
                qt, dot_t = q_h.T, do_h.T
                lse = lse_ref[i, h : h + 1, :]
                delta = jnp.sum(product[h * HD : h * HD + HD], axis=0, keepdims=True)
                dq = None
                for b in range(i + 1):
                    rows_b = rows_of(b)
                    s = jnp.dot(qkv_ref[rows_b, 128:256], qt, preferred_element_type=F32)
                    s = s * (SCALE * LOG2E) - lse
                    if b == i:
                        s = jnp.where(diagonal_mask(i, length), s, NEG)
                    p = jnp.exp2(s)
                    dp = jnp.dot(qkv_ref[rows_b, 256:384], dot_t, preferred_element_type=F32)
                    ds = (p * (dp - delta)).astype(BF)
                    dv = jnp.dot(p.astype(BF), do_h, preferred_element_type=F32)
                    dk = jnp.dot(ds, q_h, preferred_element_type=F32)
                    if b == i and h == 0:
                        dv_ref[b] = dv
                        dk_ref[b] = dk
                    else:
                        dv_ref[b] += dv
                        dk_ref[b] += dk
                    part = jnp.dot(kt_ref[b, h * HD : h * HD + HD, :], ds, preferred_element_type=F32)
                    dq = part if dq is None else dq + part
                dq_t.append(rope_back(dq * SCALE, cos_ref[i], sin_ref[i]))
            d_ref[where_q, 0:128] = jnp.concatenate(dq_t, axis=0).T.astype(BF)

        @pl.when(i * BLK >= length)
        def _():
            d_ref[rows_of(i), :] = jnp.zeros((BLK, 384), BF)

    for i in range(count):

        @pl.when(i * BLK < length)
        def _():
            where_k = rows_of(i)
            dk_t = dk_ref[i].T * SCALE
            parts = [rope_back(dk_t[h * HD : h * HD + HD], cos_ref[i], sin_ref[i]) for h in range(2)]
            d_ref[where_k, 128:256] = jnp.concatenate(parts, axis=0).T.astype(BF)
            d_ref[where_k, 256:384] = dv_ref[i].astype(BF)


def attend_back(info, qkv, mixed, grad_mixed, lse, cos_t, sin_t, group):
    seq, cols = qkv.shape
    pairs = cols // 384
    count = seq // BLK
    return pl.pallas_call(
        functools.partial(attend_back_kernel, group),
        grid_spec=pltpu.PrefetchScalarGridSpec(
            num_scalar_prefetch=1,
            grid=(pairs,),
            in_specs=[
                pl.BlockSpec((seq, 384), lambda p, s: (0, p)),
                pl.BlockSpec((seq, 128), lambda p, s: (0, p)),
                pl.BlockSpec((seq, 128), lambda p, s: (0, p)),
                pl.BlockSpec((None, count, 2, BLK), lambda p, s: (p, 0, 0, 0)),
                pl.BlockSpec((count, HD // 2, BLK), lambda p, s: (0, 0, 0)),
                pl.BlockSpec((count, HD // 2, BLK), lambda p, s: (0, 0, 0)),
            ],
            out_specs=pl.BlockSpec((seq, 384), lambda p, s: (0, p)),
            scratch_shapes=[
                pltpu.VMEM((count, 128, BLK), BF),
                pltpu.VMEM((count, BLK, 128), F32),
                pltpu.VMEM((count, BLK, 128), F32),
            ],
        ),
        out_shape=jax.ShapeDtypeStruct((seq, cols), BF),
        compiler_params=pltpu.CompilerParams(vmem_limit_bytes=VMEM_BYTES),
        cost_estimate=pl.CostEstimate(
            flops=pairs * 2 * seq * seq * 5 * 256, bytes_accessed=2 * seq * pairs * 1024, transcendentals=pairs * seq * seq
        ),
        name="attend_back",
    )(info, qkv, mixed, grad_mixed, lse, cos_t, sin_t)


def norm_forward(residual, gain_vec):
    factor = lax.rsqrt(jnp.mean(residual * residual, axis=-1, keepdims=True) + NORM_EPS)
    return residual * factor * gain_vec, factor


def norm_backward(residual, factor, gain_vec, grad_in):
    scaled = grad_in * gain_vec
    grad_resid = factor * scaled - residual * factor**3 * jnp.mean(scaled * residual, axis=-1, keepdims=True)
    grad_gain = jnp.sum(grad_in * residual * factor, axis=(0, 1))
    return grad_resid, grad_gain


def mul_nn(a, b):
    return jnp.dot(a, b, preferred_element_type=F32)


def mul_nt(a, b):
    return lax.dot_general(a, b, (((1,), (1,)), ((), ())), preferred_element_type=F32)


def mul_tn(a, b):
    return lax.dot_general(a, b, (((0,), (0,)), ((), ())), preferred_element_type=F32)


def after(value, *anchors):
    return lax.optimization_barrier((value, *anchors))[0]


def local(inputs, out_grad, lengths, norm1_gain, qkv_weight, out_weight, norm2_gain, gate_up_weight, down_weight):
    rows, dim = inputs.shape[2:]
    group = lax.axis_size("tp")
    seq = SEG * group * rows
    seg, fsdp, me = lax.axis_index("seg"), lax.axis_index("fsdp"), lax.axis_index("tp")
    length = jnp.sum(
        jnp.where(
            (jnp.arange(lengths.shape[0])[:, None] == seg) & (jnp.arange(lengths.shape[1])[None] == fsdp), lengths, 0
        )
    )

    def to_own(stacked):
        mine = lax.dynamic_index_in_dim(stacked[:, 0], seg, 0, keepdims=False)
        other = lax.dynamic_index_in_dim(stacked[:, 0], 1 - seg, 0, keepdims=False)
        got = swap(other, "seg", 1)
        return jnp.where(seg == 0, jnp.stack([mine, got]), jnp.stack([got, mine]))

    def from_own(own):
        mine = lax.dynamic_index_in_dim(own, seg, 0, keepdims=False)
        other = lax.dynamic_index_in_dim(own, 1 - seg, 0, keepdims=False)
        got = swap(other, "seg", 1)
        return jnp.where(seg == 0, jnp.stack([mine, got]), jnp.stack([got, mine]))[:, None]

    def both(shard):
        return jnp.stack([shard, swap(shard, "seg", 1)], axis=-2)

    def rows_full(shard):
        return lax.all_gather(shard, "fsdp", axis=0, tiled=True)

    depth = qkv_weight.shape[0]
    head_cols = qkv_weight.shape[2]
    pairs = SEG * head_cols // 128
    ff = down_weight.shape[0]
    w_qkv = both(qkv_weight).reshape(depth, 3, pairs, 128).transpose(0, 2, 1, 3).reshape(depth, pairs * 384)
    w_qkv = rows_full(w_qkv)
    gains = lax.all_gather(jnp.stack([norm1_gain, norm2_gain]), "fsdp", axis=0).astype(F32)
    gain_one = gains[:, 0].reshape(-1)
    gain_two = gains[:, 1].reshape(-1)
    residual = to_own(inputs).astype(F32)
    w_out = rows_full(after(both(out_weight.T).reshape(depth, SEG * head_cols), w_qkv))
    w_gate_up = rows_full(after(both(gate_up_weight).reshape(depth, 2 * SEG * ff), w_out))
    w_down = rows_full(after(both(down_weight.T).reshape(depth, SEG * ff), w_gate_up))

    slot = jnp.arange(group)
    position = (
        jnp.arange(SEG)[:, None, None] * (group * rows)
        + jnp.bitwise_xor(slot, me)[None, :, None] * rows
        + jnp.arange(rows)[None, None, :]
    ).reshape(seq)
    inverse = ROPE_THETA ** (-(jnp.arange(HD // 2).astype(F32) * 2.0) / HD)
    angles = position.astype(F32)[:, None] * inverse[None, :]
    cos, sin = jnp.cos(angles), jnp.sin(angles)
    zero = jnp.zeros_like(sin)
    cos_tab = jnp.concatenate([cos] * 4, axis=1)
    sin_a = jnp.concatenate([-sin, zero, -sin, zero], axis=1)
    sin_b = jnp.concatenate([zero, sin, zero, sin], axis=1)
    natural = jnp.arange(seq).astype(F32)
    angles_t = inverse[None, :, None] * natural.reshape(seq // BLK, 1, BLK)
    cos_t, sin_t = jnp.cos(angles_t), jnp.sin(angles_t)
    in_kernel = rows == BLK
    info = jnp.stack([length, me if in_kernel else jnp.int32(0)]).astype(jnp.int32)
    kernel_group = group if in_kernel else 1

    def reorder(full):
        if in_kernel:
            return full
        split = full.reshape(SEG, group, rows, full.shape[-1])
        return jnp.take(split, jnp.bitwise_xor(slot, me), axis=1).reshape(full.shape)

    own_position = (
        jnp.arange(SEG)[:, None, None] * (group * rows) + me * rows + jnp.arange(rows)[None, :, None]
    )
    live = (own_position < length).astype(F32)

    normed, factor_one = norm_forward(residual, gain_one)
    normed_rows = gather_rows(normed.astype(BF))
    qkv = reorder(qkv_project(normed_rows, w_qkv, cos_tab, sin_a, sin_b))
    mixed, lse = attend(info, qkv, kernel_group)
    mixed_slots = reorder(mixed)
    middle = residual + scatter_rows(mul_nt(mixed_slots, w_out).astype(BF), rows)
    normed_two, factor_two = norm_forward(middle, gain_two)
    two_rows = gather_rows(normed_two.astype(BF))

    grad_result = to_own(out_grad).astype(F32) * live
    grad_rows = gather_rows(grad_result.astype(BF))

    half_ff = SEG * ff
    gate = mul_nn(two_rows, w_gate_up[:, :half_ff]).astype(BF)
    upward = mul_nn(two_rows, w_gate_up[:, half_ff:]).astype(BF)
    gate32, up32 = gate.astype(F32), upward.astype(F32)
    sig = jax.nn.sigmoid(gate32)
    hidden = (gate32 * sig * up32).astype(BF)
    result = middle + scatter_rows(mul_nt(hidden, w_down).astype(BF), rows)
    outputs = from_own((result * live).astype(BF))

    grad_hidden = mul_nn(grad_rows, w_down)
    grad_gate = grad_hidden * up32 * sig * (1.0 + gate32 * (1.0 - sig))
    grad_up = grad_hidden * gate32 * sig
    grad_gate_up = jnp.concatenate([grad_gate.astype(BF), grad_up.astype(BF)], axis=1)
    grad_two = scatter_rows(mul_nt(grad_gate_up, w_gate_up).astype(BF), rows)

    def reduce_rows(full, anchor=None):
        full = full.astype(BF)
        if anchor is not None:
            full = after(full, anchor)
        return lax.psum_scatter(full, "fsdp", scatter_dimension=0, tiled=True)

    def reduce_seg(part):
        return part[..., 0, :].astype(F32) + swap(part[..., 1, :], "seg", 1).astype(F32)

    down_part = reduce_rows(mul_tn(grad_rows, hidden))
    gate_up_part = reduce_rows(mul_tn(two_rows, grad_gate_up))
    grad_resid_two, grad_gain_two = norm_backward(middle, factor_two, gain_two, grad_two)
    grad_middle = grad_result + grad_resid_two
    mid_rows = gather_rows(grad_middle.astype(BF))
    out_part = reduce_rows(mul_tn(mid_rows, mixed_slots))
    grad_mixed = reorder(mul_nn(mid_rows, w_out).astype(BF))
    grad_raw = reorder(attend_back(info, qkv, mixed, grad_mixed, lse, cos_t, sin_t, kernel_group))
    qkv_part = reduce_rows(mul_tn(normed_rows, grad_raw))
    grad_one = scatter_rows(mul_nt(grad_raw, w_qkv).astype(BF), rows)
    grad_resid_one, grad_gain_one = norm_backward(residual, factor_one, gain_one, grad_one)
    input_grad = from_own((grad_middle + grad_resid_one).astype(BF))

    grad_down = reduce_seg(down_part.reshape(depth, SEG, ff)).T
    grad_gu = reduce_seg(gate_up_part.reshape(depth, 2, SEG, ff))
    grad_out = reduce_seg(out_part.reshape(depth, SEG, head_cols)).T
    qkv_part = qkv_part.reshape(depth, pairs, 3, 128).transpose(0, 2, 1, 3)
    grad_qkv = reduce_seg(qkv_part.reshape(depth, 3, SEG, head_cols))
    gain_sums = lax.psum(jnp.stack([grad_gain_one, grad_gain_two]), ("fsdp", "seg", "tp"))
    gain_own = lax.dynamic_slice_in_dim(gain_sums, fsdp * depth, depth, axis=1)
    return (outputs, input_grad, gain_own[0], grad_qkv, grad_out, gain_own[1], grad_gu, grad_down)


def solution(mesh):
    fsdp, tp = mesh.devices.shape
    inner = Mesh(mesh.devices.reshape(fsdp, SEG, tp // SEG), ("fsdp", "seg", "tp"))
    act = P(None, "fsdp", ("seg", "tp"), None)
    col = P("fsdp", None, ("seg", "tp"))
    row = P(("seg", "tp"), "fsdp")
    return jax.shard_map(
        local,
        mesh=inner,
        in_specs=(act, act, P(), P("fsdp"), col, row, P("fsdp"), col, row),
        out_specs=(act, act, P("fsdp"), col, row, P("fsdp"), col, row),
        check_vma=False,
    )
```

```python
import functools
import math

import jax
import jax.numpy as jnp
from jax import lax
from jax.experimental import pallas as pl
from jax.experimental.pallas import tpu as pltpu
from jax.sharding import Mesh
from jax.sharding import PartitionSpec as P


HD = 64
NORM_EPS = 1e-05
ROPE_THETA = 130000.0
BLK = 256
SEG = 2
BF = jnp.bfloat16
F32 = jnp.float32
NEG = -1e30
SCALE = 1.0 / math.sqrt(HD)
LOG2E = math.log2(math.e)
VMEM_BYTES = 60 * 1024 * 1024


OWN, OTHER = 0, 1


def swap(x, axis, bit):
    size = lax.axis_size(axis)
    return lax.ppermute(x, axis, [(i, i ^ bit) for i in range(size)])


def gather_slots(x, axis):
    size = lax.axis_size(axis)
    slots = {0: x}
    bit = size // 2
    while bit:
        for k in list(slots):
            slots[k | bit] = swap(slots[k], axis, bit)
        bit //= 2
    return [slots[k] for k in range(size)]


def scatter_slots(parts, axis):
    slots = dict(enumerate(parts))
    bit = 1
    while bit < lax.axis_size(axis):
        for k in [k for k in slots if k & bit]:
            got = swap(slots.pop(k), axis, bit)
            kept = slots[k ^ bit].astype(F32) + got.astype(F32)
            slots[k ^ bit] = kept if bit * 2 == lax.axis_size(axis) else kept.astype(BF)
        bit *= 2
    return slots[0]


def gather_rows(local):
    blocks = gather_slots(local, "tp")
    return jnp.concatenate([b[h] for h in range(2) for b in blocks], axis=0)


def scatter_rows(full, rows):
    size = lax.axis_size("tp")
    parts = full.reshape(2, size, rows, full.shape[-1])
    return scatter_slots([parts[:, k] for k in range(size)], "tp")


def scatter_half(half, rows):
    parts = half.reshape(-1, rows, half.shape[-1])
    return scatter_slots([parts[k] for k in range(parts.shape[0])], "tp")


def sum_all(x, axes):
    for axis in axes:
        bit = 1
        while bit < lax.axis_size(axis):
            x = x + swap(x, axis, bit)
            bit *= 2
    return x


def qkv_kernel(x_ref, w_ref, cos_ref, sa_ref, sb_ref, o_ref):
    acc = jnp.dot(x_ref[...], w_ref[...], preferred_element_type=F32)
    cos, sin_a, sin_b = cos_ref[...], sa_ref[...], sb_ref[...]
    for part in range(o_ref.shape[1] // 128):
        lanes = slice(part * 128, part * 128 + 128)
        u = acc[:, lanes]
        if part % 3 < 2:
            u = u * cos + pltpu.roll(u, 96, 1) * sin_a + pltpu.roll(u, 32, 1) * sin_b
        o_ref[:, lanes] = u.astype(BF)


def qkv_project(rows, weight, cos, sin_a, sin_b):
    seq, dim = rows.shape
    cols = weight.shape[1] // 4 * 3
    row_block = min(BLK, seq)
    return pl.pallas_call(
        qkv_kernel,
        grid=(seq // row_block,),
        in_specs=[
            pl.BlockSpec((row_block, dim), lambda i: (i, 0)),
            pl.BlockSpec((dim, cols), lambda i: (0, 0), pipeline_mode=pl.Buffered(1)),
        ]
        + [pl.BlockSpec((row_block, 128), lambda i: (i, 0))] * 3,
        out_specs=pl.BlockSpec((row_block, cols), lambda i: (i, 0)),
        out_shape=jax.ShapeDtypeStruct((seq, cols), BF),
        compiler_params=pltpu.CompilerParams(vmem_limit_bytes=VMEM_BYTES),
        cost_estimate=pl.CostEstimate(
            flops=2 * seq * dim * cols, bytes_accessed=2 * (seq * dim + dim * cols + seq * cols), transcendentals=0
        ),
        name="qkv_project",
    )(rows, weight, cos, sin_a, sin_b)


def slot_of(block, group, turn, side):
    return jnp.bitwise_xor(block // group, side) * group + jnp.bitwise_xor(block % group, turn)


def lane_masks(rows):
    lane = lax.broadcasted_iota(jnp.int32, (rows, 128), 1)
    return lane < HD, lane >= HD


def diagonal_mask(block, length):
    key = lax.broadcasted_iota(jnp.int32, (BLK, BLK), 0)
    query = lax.broadcasted_iota(jnp.int32, (BLK, BLK), 1)
    return (key <= query) & (key + block * BLK < length)


def attend_kernel(group, info_ref, qkv_ref, o_ref, lse_ref, vt_ref):
    count = qkv_ref.shape[0] // BLK
    length, turn, side = info_ref[0], info_ref[1], info_ref[2]

    def rows_of(block):
        return pl.ds(pl.multiple_of(slot_of(block, group, turn, side) * BLK, BLK), BLK)

    masks = lane_masks(BLK)
    for i in range(count):

        @pl.when(i * BLK < length)
        def _():
            where_q = rows_of(i)
            vt_ref[i] = qkv_ref[where_q, 256:384].T
            q = qkv_ref[where_q, 0:128]
            outs = []
            for h in range(2):
                qt = jnp.where(masks[h], q, jnp.zeros_like(q)).T
                top = total = acc = None
                step = 2
                first = 0
                while first <= i:
                    blocks = list(range(first, min(first + step, i + 1)))
                    scores = []
                    for b in blocks:
                        s = jnp.dot(qkv_ref[rows_of(b), 128:256], qt, preferred_element_type=F32) * (SCALE * LOG2E)
                        if b == i:
                            s = jnp.where(diagonal_mask(i, length), s, NEG)
                        scores.append(s)
                    new_top = functools.reduce(jnp.maximum, [jnp.max(s, axis=0, keepdims=True) for s in scores])
                    if top is not None:
                        new_top = jnp.maximum(top, new_top)
                        fade = jnp.exp2(top - new_top)
                        total, acc = total * fade, acc * fade
                    for b, s in zip(blocks, scores):
                        p = jnp.exp2(s - new_top)
                        p_sum = jnp.sum(p, axis=0, keepdims=True)
                        mixed = jnp.dot(
                            vt_ref[b, h * HD : h * HD + HD, :], p.astype(BF), preferred_element_type=F32
                        )
                        total = p_sum if total is None else total + p_sum
                        acc = mixed if acc is None else acc + mixed
                    top = new_top
                    first += step
                outs.append(acc / total)
                lse_ref[i, h : h + 1, :] = top + jnp.log2(total)
            o_ref[where_q, :] = jnp.concatenate(outs, axis=0).T.astype(BF)

        @pl.when(i * BLK >= length)
        def _():
            o_ref[rows_of(i), :] = jnp.zeros((BLK, 128), BF)
            lse_ref[i] = jnp.zeros((2, BLK), F32)


def attend(info, qkv, group):
    seq, cols = qkv.shape
    pairs = cols // 384
    count = seq // BLK
    return pl.pallas_call(
        functools.partial(attend_kernel, group),
        grid_spec=pltpu.PrefetchScalarGridSpec(
            num_scalar_prefetch=1,
            grid=(pairs,),
            in_specs=[pl.BlockSpec((seq, 384), lambda p, s: (0, p))],
            out_specs=[
                pl.BlockSpec((seq, 128), lambda p, s: (0, p)),
                pl.BlockSpec((None, count, 2, BLK), lambda p, s: (p, 0, 0, 0)),
            ],
            scratch_shapes=[pltpu.VMEM((count, 128, BLK), BF)],
        ),
        out_shape=[
            jax.ShapeDtypeStruct((seq, pairs * 128), BF),
            jax.ShapeDtypeStruct((pairs, count, 2, BLK), F32),
        ],
        compiler_params=pltpu.CompilerParams(vmem_limit_bytes=VMEM_BYTES),
        cost_estimate=pl.CostEstimate(
            flops=pairs * 2 * seq * seq * 2 * 256, bytes_accessed=2 * seq * pairs * 512, transcendentals=pairs * seq * seq
        ),
        name="attend",
    )(info, qkv)


def rope_back(w, cos_t, sin_t):
    half = HD // 2
    upper, lower = w[:half], w[half:]
    return jnp.concatenate([upper * cos_t + lower * sin_t, lower * cos_t - upper * sin_t], axis=0)


def attend_back_kernel(
    group, info_ref, qkv_ref, o_ref, do_ref, lse_ref, cos_ref, sin_ref, d_ref, kt_ref, dk_ref, dv_ref
):
    count = qkv_ref.shape[0] // BLK
    length, turn, side = info_ref[0], info_ref[1], info_ref[2]

    def rows_of(block):
        return pl.ds(pl.multiple_of(slot_of(block, group, turn, side) * BLK, BLK), BLK)

    masks = lane_masks(BLK)
    for i in range(count):

        @pl.when(i * BLK < length)
        def _():
            where_q = rows_of(i)
            kt_ref[i] = qkv_ref[where_q, 128:256].T
            q = qkv_ref[where_q, 0:128]
            do = do_ref[where_q, :]
            product = (o_ref[where_q, :].astype(F32) * do.astype(F32)).T
            zero = jnp.zeros_like(q)
            dq_t = []
            for h in range(2):
                q_h = jnp.where(masks[h], q, zero)
                do_h = jnp.where(masks[h], do, zero)
                qt, dot_t = q_h.T, do_h.T
                lse = lse_ref[i, h : h + 1, :]
                delta = jnp.sum(product[h * HD : h * HD + HD], axis=0, keepdims=True)
                dq = None
                for b in range(i + 1):
                    rows_b = rows_of(b)
                    s = jnp.dot(qkv_ref[rows_b, 128:256], qt, preferred_element_type=F32)
                    s = s * (SCALE * LOG2E) - lse
                    if b == i:
                        s = jnp.where(diagonal_mask(i, length), s, NEG)
                    p = jnp.exp2(s)
                    dp = jnp.dot(qkv_ref[rows_b, 256:384], dot_t, preferred_element_type=F32)
                    ds = (p * (dp - delta)).astype(BF)
                    dv = jnp.dot(p.astype(BF), do_h, preferred_element_type=F32)
                    dk = jnp.dot(ds, q_h, preferred_element_type=F32)
                    if b == i and h == 0:
                        dv_ref[b] = dv
                        dk_ref[b] = dk
                    else:
                        dv_ref[b] += dv
                        dk_ref[b] += dk
                    part = jnp.dot(kt_ref[b, h * HD : h * HD + HD, :], ds, preferred_element_type=F32)
                    dq = part if dq is None else dq + part
                dq_t.append(rope_back(dq * SCALE, cos_ref[i], sin_ref[i]))
            d_ref[where_q, 0:128] = jnp.concatenate(dq_t, axis=0).T.astype(BF)

        @pl.when(i * BLK >= length)
        def _():
            d_ref[rows_of(i), :] = jnp.zeros((BLK, 384), BF)

    for i in range(count):

        @pl.when(i * BLK < length)
        def _():
            where_k = rows_of(i)
            dk_t = dk_ref[i].T * SCALE
            parts = [rope_back(dk_t[h * HD : h * HD + HD], cos_ref[i], sin_ref[i]) for h in range(2)]
            d_ref[where_k, 128:256] = jnp.concatenate(parts, axis=0).T.astype(BF)
            d_ref[where_k, 256:384] = dv_ref[i].astype(BF)


def attend_back(info, qkv, mixed, grad_mixed, lse, cos_t, sin_t, group):
    seq, cols = qkv.shape
    pairs = cols // 384
    count = seq // BLK
    return pl.pallas_call(
        functools.partial(attend_back_kernel, group),
        grid_spec=pltpu.PrefetchScalarGridSpec(
            num_scalar_prefetch=1,
            grid=(pairs,),
            in_specs=[
                pl.BlockSpec((seq, 384), lambda p, s: (0, p)),
                pl.BlockSpec((seq, 128), lambda p, s: (0, p)),
                pl.BlockSpec((seq, 128), lambda p, s: (0, p)),
                pl.BlockSpec((None, count, 2, BLK), lambda p, s: (p, 0, 0, 0)),
                pl.BlockSpec((count, HD // 2, BLK), lambda p, s: (0, 0, 0)),
                pl.BlockSpec((count, HD // 2, BLK), lambda p, s: (0, 0, 0)),
            ],
            out_specs=pl.BlockSpec((seq, 384), lambda p, s: (0, p)),
            scratch_shapes=[
                pltpu.VMEM((count, 128, BLK), BF),
                pltpu.VMEM((count, BLK, 128), F32),
                pltpu.VMEM((count, BLK, 128), F32),
            ],
        ),
        out_shape=jax.ShapeDtypeStruct((seq, pairs * 384), BF),
        compiler_params=pltpu.CompilerParams(vmem_limit_bytes=VMEM_BYTES),
        cost_estimate=pl.CostEstimate(
            flops=pairs * 2 * seq * seq * 5 * 256, bytes_accessed=2 * seq * pairs * 1024, transcendentals=pairs * seq * seq
        ),
        name="attend_back",
    )(info, qkv, mixed, grad_mixed, lse, cos_t, sin_t)


def norm_forward(residual, gain_vec):
    factor = lax.rsqrt(jnp.mean(residual * residual, axis=-1, keepdims=True) + NORM_EPS)
    return residual * factor * gain_vec, factor


def norm_backward(residual, factor, gain_vec, grad_in):
    scaled = grad_in * gain_vec
    grad_resid = factor * scaled - residual * factor**3 * jnp.mean(scaled * residual, axis=-1, keepdims=True)
    grad_gain = jnp.sum(grad_in * residual * factor, axis=tuple(range(grad_in.ndim - 1)))
    return grad_resid, grad_gain


def mul(a, b, dims):
    return lax.dot_general(a, b, (dims, ((), ())), preferred_element_type=F32)


NN, NT, TN = ((1,), (0,)), ((1,), (1,)), ((0,), (0,))


def after(value, *anchors):
    return lax.optimization_barrier((value, *anchors))[0]


def layer(inputs, out_grad, lengths, norm1_gain, qkv_weight, out_weight, norm2_gain, gate_up_weight, down_weight):
    rows, _ = inputs.shape[2:]
    group = lax.axis_size("tp")
    seq = SEG * group * rows
    seg, fsdp, me = lax.axis_index("seg"), lax.axis_index("fsdp"), lax.axis_index("tp")
    length = jnp.sum(
        jnp.where(
            (jnp.arange(lengths.shape[0])[:, None] == seg) & (jnp.arange(lengths.shape[1])[None] == fsdp), lengths, 0
        )
    )

    def parted(stacked):
        mine = lax.dynamic_index_in_dim(stacked[:, 0], seg, 0, keepdims=False)
        other = lax.dynamic_index_in_dim(stacked[:, 0], 1 - seg, 0, keepdims=False)
        return mine, other

    def joined(mine, got):
        return jnp.where(seg == 0, jnp.stack([mine, got]), jnp.stack([got, mine]))[:, None]

    def rows_full(shard):
        return lax.all_gather(shard, "fsdp", axis=0, tiled=True)

    def wide(shard):
        return [rows_full(shard), rows_full(swap(shard, "seg", 1))]

    depth = qkv_weight.shape[0]
    head_cols = qkv_weight.shape[2]
    ff = down_weight.shape[0]
    whole_pairs = head_cols % 128 == 0

    def paired(qkv_cols, out_cols):
        count = out_cols.shape[1] // 128
        by_pair = qkv_cols.reshape(depth, 3, count, 128).transpose(0, 2, 1, 3).reshape(depth, count * 384)
        return jnp.concatenate([by_pair, out_cols], axis=1)

    def unpaired(joint):
        count = joint.shape[1] // 512
        by_pair = joint[:, : count * 384].reshape(depth, count, 3, 128).transpose(0, 2, 1, 3)
        return by_pair.reshape(depth, 3, count * 128), joint[:, count * 384 :]

    x_mine, x_other = parted(inputs)
    x_got = swap(x_other, "seg", 1)
    if whole_pairs:
        w_qkvo = wide(paired(qkv_weight, out_weight.T))
    else:
        both = [jnp.stack([w, swap(w, "seg", 1)], axis=-2) for w in (qkv_weight, out_weight.T)]
        w_qkvo = [rows_full(paired(both[0].reshape(depth, 3, -1), both[1].reshape(depth, -1)))]
    gains = lax.all_gather(jnp.stack([norm1_gain, norm2_gain]), "fsdp", axis=0).astype(F32)
    gain_one = gains[:, 0].reshape(-1)
    gain_two = gains[:, 1].reshape(-1)
    w_down = wide(down_weight.T)
    w_gu = wide(gate_up_weight.reshape(depth, 2 * ff))
    cut = w_qkvo[0].shape[1] // 4 * 3
    w_out = jnp.concatenate([w[:, cut:] for w in w_qkvo], axis=1)

    slot = jnp.arange(group)
    position = (
        jnp.bitwise_xor(jnp.arange(SEG), seg)[:, None, None] * (group * rows)
        + jnp.bitwise_xor(slot, me)[None, :, None] * rows
        + jnp.arange(rows)[None, None, :]
    ).reshape(seq)
    inverse = ROPE_THETA ** (-(jnp.arange(HD // 2).astype(F32) * 2.0) / HD)
    angles = position.astype(F32)[:, None] * jnp.tile(inverse, 4)[None, :]
    cos_tab, sin = jnp.cos(angles), jnp.sin(angles)
    first = (jnp.arange(128) % HD < HD // 2)[None, :]
    sin_a = jnp.where(first, -sin, 0.0)
    sin_b = jnp.where(first, 0.0, sin)
    natural = jnp.arange(seq).astype(F32)
    angles_t = inverse[None, :, None] * natural.reshape(seq // BLK, 1, BLK)
    cos_t, sin_t = jnp.cos(angles_t), jnp.sin(angles_t)
    in_kernel = rows == BLK
    none = jnp.int32(0)
    info = jnp.stack([length, me if in_kernel else none, seg if in_kernel else none]).astype(jnp.int32)
    kernel_group = group if in_kernel else seq // BLK // SEG

    def reorder(full):
        if in_kernel:
            return full
        split = full.reshape(SEG, group, rows, full.shape[-1])
        split = jnp.take(split, jnp.bitwise_xor(jnp.arange(SEG), seg), axis=0)
        return jnp.take(split, jnp.bitwise_xor(slot, me), axis=1).reshape(full.shape)

    own_position = (
        jnp.bitwise_xor(jnp.arange(SEG), seg)[:, None, None] * (group * rows)
        + me * rows
        + jnp.arange(rows)[None, :, None]
    )
    live = (own_position < length).astype(F32)

    halves = [x_mine.astype(F32), x_got.astype(F32)]
    blocks, factor_one = [], []
    for x in halves:
        normed, factor = norm_forward(x, gain_one)
        blocks.append(gather_slots(normed.astype(BF), "tp"))
        factor_one.append(factor)
    normed_rows = jnp.concatenate(blocks[0] + blocks[1], axis=0)
    residual = jnp.stack(halves)
    qkv, mixed, lse = [], [], []
    for part, weight in enumerate(w_qkvo):
        projected = qkv_project(normed_rows, weight, cos_tab, sin_a, sin_b)
        qkv.append(reorder(projected))
        outs = attend(info, qkv[part], kernel_group)
        mixed.append(outs[0])
        lse.append(outs[1])
    mixed_slots = [reorder(m) for m in mixed]
    product = mul(jnp.concatenate(mixed_slots, axis=1), w_out, NT).astype(BF)
    middle = residual + scatter_rows(product, rows)
    normed_two, factor_two = norm_forward(middle, gain_two)
    two_rows = gather_rows(normed_two.astype(BF))

    g_mine, g_other = parted(out_grad)
    g_got = swap(g_other, "seg", 1)
    grad_result = jnp.stack([g_mine, g_got]).astype(F32) * live
    grad_rows = gather_rows(grad_result.astype(BF))

    gates, ups, hidden = [], [], []
    for c in range(2):
        gate = mul(two_rows, w_gu[c][:, :ff], NN).astype(BF)
        upward = mul(two_rows, w_gu[c][:, ff:], NN).astype(BF)
        gate32 = gate.astype(F32)
        hid = (gate32 * jax.nn.sigmoid(gate32) * upward.astype(F32)).astype(BF)
        gate, upward, hid = lax.optimization_barrier((gate, upward, hid))
        gates.append(gate)
        ups.append(upward)
        hidden.append(hid)
    product = mul(jnp.concatenate(hidden, axis=1), jnp.concatenate(w_down, axis=1), NT)
    result = middle + after(scatter_rows(product.astype(BF), rows), grad_rows)
    grad_parts = []
    for c in range(2):
        grad_hidden = mul(grad_rows, w_down[c], NN)
        gate32, up32 = gates[c].astype(F32), ups[c].astype(F32)
        sig = jax.nn.sigmoid(gate32)
        grad_gate = (grad_hidden * up32 * sig * (1.0 + gate32 * (1.0 - sig))).astype(BF)
        grad_up = (grad_hidden * gate32 * sig).astype(BF)
        grad_parts.append(jnp.concatenate([grad_gate, grad_up], axis=1))

    def reduce_rows(full):
        return lax.psum_scatter(full.astype(BF), "fsdp", scatter_dimension=0, tiled=True)

    def reduce_parts(terms):
        sums = [reduce_rows(t) for t in terms]
        return sums[OWN].astype(F32) + swap(sums[OTHER], "seg", 1).astype(F32)

    grad_down = reduce_parts([mul(grad_rows, hidden[c], TN) for c in range(2)]).T
    grad_gu = reduce_parts([mul(two_rows, grad_parts[c], TN) for c in range(2)])
    grad_gu = grad_gu.reshape(depth, 2, ff)
    half = seq // 2
    grad_middle, gain_two_terms, mid_blocks = [None, None], [], [None, None]
    for h in (1, 0):
        terms = [mul(grad_parts[c][h * half : (h + 1) * half], w_gu[c], NT) for c in range(2)]
        grad_two = scatter_half((terms[0] + terms[1]).astype(BF), rows)
        if h == 0:
            grad_two = after(grad_two, mid_blocks[1][0])
        grad_resid, gain_term = norm_backward(middle[h], factor_two[h], gain_two, grad_two)
        gain_two_terms.append(gain_term)
        grad_middle[h] = grad_result[h] + grad_resid
        mid_blocks[h] = gather_slots(lax.optimization_barrier(grad_middle[h].astype(BF)), "tp")
    mid_rows = jnp.concatenate(mid_blocks[0] + mid_blocks[1], axis=0)
    raws, qkvo_terms = {}, {}
    for part in reversed(range(len(w_qkvo))):
        grad_mixed = mul(mid_rows, w_qkvo[part][:, cut:], NN).astype(BF)
        raw = attend_back(
            info, qkv[part], mixed[part], reorder(grad_mixed), lse[part], cos_t, sin_t, kernel_group
        )
        raws[part] = reorder(raw)
        term = mul(normed_rows, raws[part], TN).astype(BF)
        out_term = mul(mid_rows, mixed_slots[part], TN).astype(BF)
        qkvo_terms[part] = jnp.concatenate([term, out_term], axis=1)
    if whole_pairs:
        grad_qkv, grad_out = unpaired(reduce_parts([qkvo_terms[0], qkvo_terms[1]]))
    else:
        part_qkv, part_out = unpaired(reduce_rows(qkvo_terms[0]))
        part_qkv, part_out = part_qkv.reshape(depth, 3, SEG, head_cols), part_out.reshape(depth, SEG, head_cols)
        grad_qkv, grad_out = [
            p[..., 0, :].astype(F32) + swap(p[..., 1, :], "seg", 1).astype(F32) for p in (part_qkv, part_out)
        ]
    grad_out = grad_out.T
    weight = jnp.concatenate([w[:, :cut] for w in w_qkvo], axis=1)
    input_grads, gain_terms = [None, None], []
    for h in (1, 0):
        raw = jnp.concatenate([raws[part][h * half : (h + 1) * half] for part in range(len(w_qkvo))], axis=1)
        product = mul(raw, weight, NT).astype(BF)
        grad_one = scatter_half(product, rows)
        if h == 0:
            grad_one = after(grad_one, input_grads[1])
        grad_resid, gain_term = norm_backward(halves[h], factor_one[h], gain_one, grad_one)
        gain_terms.append(gain_term)
        input_grads[h] = (grad_middle[h] + grad_resid).astype(BF)
    input_grad = joined(input_grads[0], swap(input_grads[1], "seg", 1))
    result_live = (result * live).astype(BF)
    outputs = joined(result_live[0], swap(result_live[1], "seg", 1))
    gains = jnp.stack([gain_terms[0] + gain_terms[1], gain_two_terms[0] + gain_two_terms[1]])
    gains = sum_all(gains, ("fsdp", "tp", "seg"))
    gain_one_grad, gain_two_grad = lax.dynamic_slice_in_dim(gains, fsdp * depth, depth, axis=1)
    return (outputs, input_grad, gain_one_grad, grad_qkv, grad_out, gain_two_grad, grad_gu, grad_down)


def solution(mesh):
    fsdp, tp = mesh.devices.shape
    inner = Mesh(mesh.devices.reshape(fsdp, SEG, tp // SEG), ("fsdp", "seg", "tp"))
    act = P(None, "fsdp", ("seg", "tp"), None)
    col = P("fsdp", None, ("seg", "tp"))
    row = P(("seg", "tp"), "fsdp")
    return jax.shard_map(
        layer,
        mesh=inner,
        in_specs=(act, act, P(), P("fsdp"), col, row, P("fsdp"), col, row),
        out_specs=(act, act, P("fsdp"), col, row, P("fsdp"), col, row),
        check_vma=False,
    )
```

```python
import functools
import math

import jax
import jax.numpy as jnp
from jax import lax
from jax.experimental import pallas as pl
from jax.experimental.pallas import tpu as pltpu
from jax.sharding import Mesh
from jax.sharding import PartitionSpec as P


HD = 64
NORM_EPS = 1e-05
ROPE_THETA = 130000.0
BLK = 256
SEG = 2
BF = jnp.bfloat16
F32 = jnp.float32
NEG = -1e30
SCALE = 1.0 / math.sqrt(HD)
LOG2E = math.log2(math.e)
VMEM_BYTES = 60 * 1024 * 1024


OWN, OTHER = 0, 1


def swap(x, axis, bit):
    size = lax.axis_size(axis)
    return lax.ppermute(x, axis, [(i, i ^ bit) for i in range(size)])


def gather_slots(x, axis):
    size = lax.axis_size(axis)
    slots = {0: x}
    bit = size // 2
    while bit:
        for k in list(slots):
            slots[k | bit] = swap(slots[k], axis, bit)
        bit //= 2
    return [slots[k] for k in range(size)]


def scatter_slots(parts, axis):
    slots = dict(enumerate(parts))
    bit = 1
    while bit < lax.axis_size(axis):
        for k in [k for k in slots if k & bit]:
            got = swap(slots.pop(k), axis, bit)
            kept = slots[k ^ bit].astype(F32) + got.astype(F32)
            slots[k ^ bit] = kept if bit * 2 == lax.axis_size(axis) else kept.astype(BF)
        bit *= 2
    return slots[0]


def gather_rows(local):
    blocks = gather_slots(local, "tp")
    return jnp.concatenate([b[h] for h in range(2) for b in blocks], axis=0)


def scatter_rows(full, rows):
    size = lax.axis_size("tp")
    parts = full.reshape(2, size, rows, full.shape[-1])
    return scatter_slots([parts[:, k] for k in range(size)], "tp")


def scatter_half(half, rows):
    parts = half.reshape(-1, rows, half.shape[-1])
    return scatter_slots([parts[k] for k in range(parts.shape[0])], "tp")


def sum_all(x, axes):
    for axis in axes:
        bit = 1
        while bit < lax.axis_size(axis):
            x = x + swap(x, axis, bit)
            bit *= 2
    return x


def qkv_kernel(x_ref, w_ref, cos_ref, sa_ref, sb_ref, o_ref):
    acc = jnp.dot(x_ref[...], w_ref[...], preferred_element_type=F32)
    cos, sin_a, sin_b = cos_ref[...], sa_ref[...], sb_ref[...]
    for part in range(o_ref.shape[1] // 128):
        lanes = slice(part * 128, part * 128 + 128)
        u = acc[:, lanes]
        if part % 3 < 2:
            u = u * cos + pltpu.roll(u, 96, 1) * sin_a + pltpu.roll(u, 32, 1) * sin_b
        o_ref[:, lanes] = u.astype(BF)


def qkv_project(rows, weight, cos, sin_a, sin_b):
    seq, dim = rows.shape
    cols = weight.shape[1] // 4 * 3
    row_block = min(BLK, seq)
    return pl.pallas_call(
        qkv_kernel,
        grid=(seq // row_block,),
        in_specs=[
            pl.BlockSpec((row_block, dim), lambda i: (i, 0)),
            pl.BlockSpec((dim, cols), lambda i: (0, 0), pipeline_mode=pl.Buffered(1)),
        ]
        + [pl.BlockSpec((row_block, 128), lambda i: (i, 0))] * 3,
        out_specs=pl.BlockSpec((row_block, cols), lambda i: (i, 0)),
        out_shape=jax.ShapeDtypeStruct((seq, cols), BF),
        compiler_params=pltpu.CompilerParams(vmem_limit_bytes=VMEM_BYTES),
        cost_estimate=pl.CostEstimate(
            flops=2 * seq * dim * cols, bytes_accessed=2 * (seq * dim + dim * cols + seq * cols), transcendentals=0
        ),
        name="qkv_project",
    )(rows, weight, cos, sin_a, sin_b)


def slot_of(block, group, turn, side):
    return jnp.bitwise_xor(block // group, side) * group + jnp.bitwise_xor(block % group, turn)


def lane_masks(rows):
    lane = lax.broadcasted_iota(jnp.int32, (rows, 128), 1)
    return lane < HD, lane >= HD


def diagonal_mask(block, length):
    key = lax.broadcasted_iota(jnp.int32, (BLK, BLK), 0)
    query = lax.broadcasted_iota(jnp.int32, (BLK, BLK), 1)
    return (key <= query) & (key + block * BLK < length)


def attend_kernel(group, info_ref, qkv_ref, o_ref, lse_ref, vt_ref):
    count = qkv_ref.shape[0] // BLK
    length, turn, side = info_ref[0], info_ref[1], info_ref[2]

    def rows_of(block):
        return pl.ds(pl.multiple_of(slot_of(block, group, turn, side) * BLK, BLK), BLK)

    masks = lane_masks(BLK)
    for i in range(count):

        @pl.when(i * BLK < length)
        def _():
            where_q = rows_of(i)
            vt_ref[i] = qkv_ref[where_q, 256:384].T
            q = qkv_ref[where_q, 0:128]
            outs = []
            for h in range(2):
                qt = jnp.where(masks[h], q, jnp.zeros_like(q)).T
                top = total = acc = None
                step = 2
                first = 0
                while first <= i:
                    blocks = list(range(first, min(first + step, i + 1)))
                    scores = []
                    for b in blocks:
                        s = jnp.dot(qkv_ref[rows_of(b), 128:256], qt, preferred_element_type=F32) * (SCALE * LOG2E)
                        if b == i:
                            s = jnp.where(diagonal_mask(i, length), s, NEG)
                        scores.append(s)
                    new_top = functools.reduce(jnp.maximum, [jnp.max(s, axis=0, keepdims=True) for s in scores])
                    if top is not None:
                        new_top = jnp.maximum(top, new_top)
                        fade = jnp.exp2(top - new_top)
                        total, acc = total * fade, acc * fade
                    for b, s in zip(blocks, scores):
                        p = jnp.exp2(s - new_top)
                        p_sum = jnp.sum(p, axis=0, keepdims=True)
                        mixed = jnp.dot(
                            vt_ref[b, h * HD : h * HD + HD, :], p.astype(BF), preferred_element_type=F32
                        )
                        total = p_sum if total is None else total + p_sum
                        acc = mixed if acc is None else acc + mixed
                    top = new_top
                    first += step
                outs.append(acc / total)
                lse_ref[i, h : h + 1, :] = top + jnp.log2(total)
            o_ref[where_q, :] = jnp.concatenate(outs, axis=0).T.astype(BF)

        @pl.when(i * BLK >= length)
        def _():
            o_ref[rows_of(i), :] = jnp.zeros((BLK, 128), BF)
            lse_ref[i] = jnp.zeros((2, BLK), F32)


def attend(info, qkv, group):
    seq, cols = qkv.shape
    pairs = cols // 384
    count = seq // BLK
    return pl.pallas_call(
        functools.partial(attend_kernel, group),
        grid_spec=pltpu.PrefetchScalarGridSpec(
            num_scalar_prefetch=1,
            grid=(pairs,),
            in_specs=[pl.BlockSpec((seq, 384), lambda p, s: (0, p))],
            out_specs=[
                pl.BlockSpec((seq, 128), lambda p, s: (0, p)),
                pl.BlockSpec((None, count, 2, BLK), lambda p, s: (p, 0, 0, 0)),
            ],
            scratch_shapes=[pltpu.VMEM((count, 128, BLK), BF)],
        ),
        out_shape=[
            jax.ShapeDtypeStruct((seq, pairs * 128), BF),
            jax.ShapeDtypeStruct((pairs, count, 2, BLK), F32),
        ],
        compiler_params=pltpu.CompilerParams(vmem_limit_bytes=VMEM_BYTES),
        cost_estimate=pl.CostEstimate(
            flops=pairs * 2 * seq * seq * 2 * 256, bytes_accessed=2 * seq * pairs * 512, transcendentals=pairs * seq * seq
        ),
        name="attend",
    )(info, qkv)


def rope_back(w, cos_t, sin_t):
    half = HD // 2
    upper, lower = w[:half], w[half:]
    return jnp.concatenate([upper * cos_t + lower * sin_t, lower * cos_t - upper * sin_t], axis=0)


def attend_back_kernel(
    group, info_ref, qkv_ref, o_ref, do_ref, lse_ref, cos_ref, sin_ref, d_ref, kt_ref, dk_ref, dv_ref
):
    count = qkv_ref.shape[0] // BLK
    length, turn, side = info_ref[0], info_ref[1], info_ref[2]

    def rows_of(block):
        return pl.ds(pl.multiple_of(slot_of(block, group, turn, side) * BLK, BLK), BLK)

    masks = lane_masks(BLK)
    for i in range(count):

        @pl.when(i * BLK < length)
        def _():
            where_q = rows_of(i)
            kt_ref[i] = qkv_ref[where_q, 128:256].T
            q = qkv_ref[where_q, 0:128]
            do = do_ref[where_q, :]
            product = (o_ref[where_q, :].astype(F32) * do.astype(F32)).T
            zero = jnp.zeros_like(q)
            dq_t = []
            for h in range(2):
                q_h = jnp.where(masks[h], q, zero)
                do_h = jnp.where(masks[h], do, zero)
                qt, dot_t = q_h.T, do_h.T
                lse = lse_ref[i, h : h + 1, :]
                delta = jnp.sum(product[h * HD : h * HD + HD], axis=0, keepdims=True)
                dq = None
                for b in range(i + 1):
                    rows_b = rows_of(b)
                    s = jnp.dot(qkv_ref[rows_b, 128:256], qt, preferred_element_type=F32)
                    s = s * (SCALE * LOG2E) - lse
                    if b == i:
                        s = jnp.where(diagonal_mask(i, length), s, NEG)
                    p = jnp.exp2(s)
                    dp = jnp.dot(qkv_ref[rows_b, 256:384], dot_t, preferred_element_type=F32)
                    ds = (p * (dp - delta)).astype(BF)
                    dv = jnp.dot(p.astype(BF), do_h, preferred_element_type=F32)
                    dk = jnp.dot(ds, q_h, preferred_element_type=F32)
                    if b == i and h == 0:
                        dv_ref[b] = dv
                        dk_ref[b] = dk
                    else:
                        dv_ref[b] += dv
                        dk_ref[b] += dk
                    part = jnp.dot(kt_ref[b, h * HD : h * HD + HD, :], ds, preferred_element_type=F32)
                    dq = part if dq is None else dq + part
                dq_t.append(rope_back(dq * SCALE, cos_ref[i], sin_ref[i]))
            d_ref[where_q, 0:128] = jnp.concatenate(dq_t, axis=0).T.astype(BF)

        @pl.when(i * BLK >= length)
        def _():
            d_ref[rows_of(i), :] = jnp.zeros((BLK, 384), BF)

    for i in range(count):

        @pl.when(i * BLK < length)
        def _():
            where_k = rows_of(i)
            dk_t = dk_ref[i].T * SCALE
            parts = [rope_back(dk_t[h * HD : h * HD + HD], cos_ref[i], sin_ref[i]) for h in range(2)]
            d_ref[where_k, 128:256] = jnp.concatenate(parts, axis=0).T.astype(BF)
            d_ref[where_k, 256:384] = dv_ref[i].astype(BF)


def attend_back(info, qkv, mixed, grad_mixed, lse, cos_t, sin_t, group):
    seq, cols = qkv.shape
    pairs = cols // 384
    count = seq // BLK
    return pl.pallas_call(
        functools.partial(attend_back_kernel, group),
        grid_spec=pltpu.PrefetchScalarGridSpec(
            num_scalar_prefetch=1,
            grid=(pairs,),
            in_specs=[
                pl.BlockSpec((seq, 384), lambda p, s: (0, p)),
                pl.BlockSpec((seq, 128), lambda p, s: (0, p)),
                pl.BlockSpec((seq, 128), lambda p, s: (0, p)),
                pl.BlockSpec((None, count, 2, BLK), lambda p, s: (p, 0, 0, 0)),
                pl.BlockSpec((count, HD // 2, BLK), lambda p, s: (0, 0, 0)),
                pl.BlockSpec((count, HD // 2, BLK), lambda p, s: (0, 0, 0)),
            ],
            out_specs=pl.BlockSpec((seq, 384), lambda p, s: (0, p)),
            scratch_shapes=[
                pltpu.VMEM((count, 128, BLK), BF),
                pltpu.VMEM((count, BLK, 128), F32),
                pltpu.VMEM((count, BLK, 128), F32),
            ],
        ),
        out_shape=jax.ShapeDtypeStruct((seq, pairs * 384), BF),
        compiler_params=pltpu.CompilerParams(vmem_limit_bytes=VMEM_BYTES),
        cost_estimate=pl.CostEstimate(
            flops=pairs * 2 * seq * seq * 5 * 256, bytes_accessed=2 * seq * pairs * 1024, transcendentals=pairs * seq * seq
        ),
        name="attend_back",
    )(info, qkv, mixed, grad_mixed, lse, cos_t, sin_t)


def norm_forward(residual, gain_vec):
    factor = lax.rsqrt(jnp.mean(residual * residual, axis=-1, keepdims=True) + NORM_EPS)
    return residual * factor * gain_vec, factor


def norm_backward(residual, factor, gain_vec, grad_in):
    scaled = grad_in * gain_vec
    grad_resid = factor * scaled - residual * factor**3 * jnp.mean(scaled * residual, axis=-1, keepdims=True)
    grad_gain = jnp.sum(grad_in * residual * factor, axis=tuple(range(grad_in.ndim - 1)))
    return grad_resid, grad_gain


def mul(a, b, dims):
    return lax.dot_general(a, b, (dims, ((), ())), preferred_element_type=F32)


NN, NT, TN = ((1,), (0,)), ((1,), (1,)), ((0,), (0,))


def after(value, *anchors):
    return lax.optimization_barrier((value, *anchors))[0]


def layer(inputs, out_grad, lengths, norm1_gain, qkv_weight, out_weight, norm2_gain, gate_up_weight, down_weight):
    rows, _ = inputs.shape[2:]
    group = lax.axis_size("tp")
    seq = SEG * group * rows
    seg, fsdp, me = lax.axis_index("seg"), lax.axis_index("fsdp"), lax.axis_index("tp")
    length = jnp.sum(
        jnp.where(
            (jnp.arange(lengths.shape[0])[:, None] == seg) & (jnp.arange(lengths.shape[1])[None] == fsdp), lengths, 0
        )
    )

    def parted(stacked):
        mine = lax.dynamic_index_in_dim(stacked[:, 0], seg, 0, keepdims=False)
        other = lax.dynamic_index_in_dim(stacked[:, 0], 1 - seg, 0, keepdims=False)
        return mine, other

    def joined(mine, got):
        return jnp.where(seg == 0, jnp.stack([mine, got]), jnp.stack([got, mine]))[:, None]

    def rows_full(shard):
        return lax.all_gather(shard, "fsdp", axis=0, tiled=True)

    def wide(shard):
        return [rows_full(shard), rows_full(swap(shard, "seg", 1))]

    depth = qkv_weight.shape[0]
    head_cols = qkv_weight.shape[2]
    ff = down_weight.shape[0]
    whole_pairs = head_cols % 128 == 0

    def paired(qkv_cols, out_cols):
        count = out_cols.shape[1] // 128
        by_pair = qkv_cols.reshape(depth, 3, count, 128).transpose(0, 2, 1, 3).reshape(depth, count * 384)
        return jnp.concatenate([by_pair, out_cols], axis=1)

    def unpaired(joint):
        count = joint.shape[1] // 512
        by_pair = joint[:, : count * 384].reshape(depth, count, 3, 128).transpose(0, 2, 1, 3)
        return by_pair.reshape(depth, 3, count * 128), joint[:, count * 384 :]

    x_mine, x_other = parted(inputs)
    x_got = swap(x_other, "seg", 1)
    if whole_pairs:
        w_qkvo = wide(paired(qkv_weight, out_weight.T))
    else:
        both = [jnp.stack([w, swap(w, "seg", 1)], axis=-2) for w in (qkv_weight, out_weight.T)]
        w_qkvo = [rows_full(paired(both[0].reshape(depth, 3, -1), both[1].reshape(depth, -1)))]
    gains = lax.all_gather(jnp.stack([norm1_gain, norm2_gain]), "fsdp", axis=0).astype(F32)
    gain_one = gains[:, 0].reshape(-1)
    gain_two = gains[:, 1].reshape(-1)
    w_down = wide(down_weight.T)
    w_gu = wide(gate_up_weight.reshape(depth, 2 * ff))
    cut = w_qkvo[0].shape[1] // 4 * 3
    w_out = jnp.concatenate([w[:, cut:] for w in w_qkvo], axis=1)

    slot = jnp.arange(group)
    position = (
        jnp.bitwise_xor(jnp.arange(SEG), seg)[:, None, None] * (group * rows)
        + jnp.bitwise_xor(slot, me)[None, :, None] * rows
        + jnp.arange(rows)[None, None, :]
    ).reshape(seq)
    inverse = ROPE_THETA ** (-(jnp.arange(HD // 2).astype(F32) * 2.0) / HD)
    angles = position.astype(F32)[:, None] * jnp.tile(inverse, 4)[None, :]
    cos_tab, sin = jnp.cos(angles), jnp.sin(angles)
    first = (jnp.arange(128) % HD < HD // 2)[None, :]
    sin_a = jnp.where(first, -sin, 0.0)
    sin_b = jnp.where(first, 0.0, sin)
    natural = jnp.arange(seq).astype(F32)
    angles_t = inverse[None, :, None] * natural.reshape(seq // BLK, 1, BLK)
    cos_t, sin_t = jnp.cos(angles_t), jnp.sin(angles_t)
    in_kernel = rows == BLK
    none = jnp.int32(0)
    info = jnp.stack([length, me if in_kernel else none, seg if in_kernel else none]).astype(jnp.int32)
    kernel_group = group if in_kernel else seq // BLK // SEG

    def reorder(full):
        if in_kernel:
            return full
        split = full.reshape(SEG, group, rows, full.shape[-1])
        split = jnp.take(split, jnp.bitwise_xor(jnp.arange(SEG), seg), axis=0)
        return jnp.take(split, jnp.bitwise_xor(slot, me), axis=1).reshape(full.shape)

    own_position = (
        jnp.bitwise_xor(jnp.arange(SEG), seg)[:, None, None] * (group * rows)
        + me * rows
        + jnp.arange(rows)[None, :, None]
    )
    live = (own_position < length).astype(F32)

    halves = [x_mine.astype(F32), x_got.astype(F32)]
    blocks, factor_one = [], []
    for h, x in enumerate(halves):
        if h == 1:
            x = halves[1] = after(x_got, blocks[0][0]).astype(F32)
        normed, factor = norm_forward(x, gain_one)
        normed = lax.optimization_barrier(normed.astype(BF))
        blocks.append(gather_slots(normed, "tp"))
        factor_one.append(factor)
    normed_rows = jnp.concatenate(blocks[0] + blocks[1], axis=0)
    qkv, mixed, lse = [], [], []
    for part, weight in enumerate(w_qkvo):
        qkv_rows = qkv_project(normed_rows, weight, cos_tab, sin_a, sin_b)
        qkv.append(reorder(qkv_rows))
        outs = attend(info, qkv[part], kernel_group)
        mixed.append(outs[0])
        lse.append(outs[1])
    mixed_slots = [reorder(m) for m in mixed]
    half = seq // 2
    middle, factor_two, two_blocks = [None, None], [None, None], [None, None]
    for h in range(2):
        rows_in = jnp.concatenate([m[h * half : (h + 1) * half] for m in mixed_slots], axis=1)
        summed = scatter_half(mul(rows_in, w_out, NT).astype(BF), rows)
        if h == 1:
            summed = after(summed, two_blocks[0][0])
        middle[h] = halves[h] + summed
        normed, factor_two[h] = norm_forward(middle[h], gain_two)
        normed = lax.optimization_barrier(normed.astype(BF))
        two_blocks[h] = gather_slots(normed, "tp")
    two_rows = jnp.concatenate(two_blocks[0] + two_blocks[1], axis=0)

    g_mine, g_other = parted(out_grad)
    g_got = swap(g_other, "seg", 1)
    grad_result = jnp.stack([g_mine, g_got]).astype(F32) * live
    grad_rows = gather_rows(grad_result.astype(BF))

    gates, ups, hidden = [], [], []
    for c in range(2):
        gate = mul(two_rows, w_gu[c][:, :ff], NN).astype(BF)
        upward = mul(two_rows, w_gu[c][:, ff:], NN).astype(BF)
        gate32 = gate.astype(F32)
        hid = (gate32 * jax.nn.sigmoid(gate32) * upward.astype(F32)).astype(BF)
        gate, upward, hid = lax.optimization_barrier((gate, upward, hid))
        gates.append(gate)
        ups.append(upward)
        hidden.append(hid)
    product = mul(jnp.concatenate(hidden, axis=1), jnp.concatenate(w_down, axis=1), NT)
    projected = scatter_rows(product.astype(BF), rows)
    grad_parts = []
    for c in range(2):
        grad_hidden = mul(grad_rows, w_down[c], NN)
        gate32, up32 = gates[c].astype(F32), ups[c].astype(F32)
        sig = jax.nn.sigmoid(gate32)
        grad_gate = (grad_hidden * up32 * sig * (1.0 + gate32 * (1.0 - sig))).astype(BF)
        grad_up = (grad_hidden * gate32 * sig).astype(BF)
        grad_parts.append(jnp.concatenate([grad_gate, grad_up], axis=1))

    def reduce_rows(full):
        return lax.psum_scatter(full.astype(BF), "fsdp", scatter_dimension=0, tiled=True)

    def reduce_parts(terms):
        sums = [reduce_rows(t) for t in terms]
        return sums[OWN].astype(F32) + swap(sums[OTHER], "seg", 1).astype(F32)

    grad_down = reduce_parts([mul(grad_rows, hidden[c], TN) for c in range(2)]).T
    grad_gu = reduce_parts([mul(two_rows, grad_parts[c], TN) for c in range(2)])
    grad_gu = grad_gu.reshape(depth, 2, ff)
    grad_middle, gain_two_terms, mid_blocks = [None, None], [], [None, None]
    for h in range(2):
        weights = w_gu if h == 0 else lax.optimization_barrier(w_gu)
        grads = jnp.concatenate([g[h * half : (h + 1) * half] for g in grad_parts], axis=1)
        product = mul(grads, jnp.concatenate(weights, axis=1), NT)
        grad_two = scatter_half(product.astype(BF), rows)
        if h == 1:
            grad_two = after(grad_two, mid_blocks[0][0])
        grad_resid, gain_term = norm_backward(middle[h], factor_two[h], gain_two, grad_two)
        gain_two_terms.append(gain_term)
        grad_middle[h] = grad_result[h] + grad_resid
        mid_blocks[h] = gather_slots(lax.optimization_barrier(grad_middle[h].astype(BF)), "tp")
    mid_rows = jnp.concatenate(mid_blocks[0] + mid_blocks[1], axis=0)
    projected = after(projected, mid_blocks[1][0])
    result_live = [((middle[h] + projected[h]) * live[h]).astype(BF) for h in range(2)]
    raws, qkvo_terms = {}, {}
    for part in reversed(range(len(w_qkvo))):
        grad_mixed = mul(mid_rows, w_qkvo[part][:, cut:], NN).astype(BF)
        raw = attend_back(
            info, qkv[part], mixed[part], reorder(grad_mixed), lse[part], cos_t, sin_t, kernel_group
        )
        raws[part] = reorder(raw)
        term = mul(normed_rows, raws[part], TN).astype(BF)
        out_term = mul(mid_rows, mixed_slots[part], TN).astype(BF)
        qkvo_terms[part] = jnp.concatenate([term, out_term], axis=1)
    if whole_pairs:
        grad_qkv, grad_out = unpaired(reduce_parts([qkvo_terms[0], qkvo_terms[1]]))
    else:
        part_qkv, part_out = unpaired(reduce_rows(qkvo_terms[0]))
        part_qkv, part_out = part_qkv.reshape(depth, 3, SEG, head_cols), part_out.reshape(depth, SEG, head_cols)
        grad_qkv, grad_out = [
            p[..., 0, :].astype(F32) + swap(p[..., 1, :], "seg", 1).astype(F32) for p in (part_qkv, part_out)
        ]
    grad_out = grad_out.T
    weight = jnp.concatenate([w[:, :cut] for w in w_qkvo], axis=1)
    input_grads, gain_terms = [None, None], []
    for h in (1, 0):
        raw = jnp.concatenate([raws[part][h * half : (h + 1) * half] for part in range(len(w_qkvo))], axis=1)
        product = mul(raw, weight, NT).astype(BF)
        grad_one = scatter_half(product, rows)
        if h == 0:
            grad_one = after(grad_one, input_grads[1])
        grad_resid, gain_term = norm_backward(halves[h], factor_one[h], gain_one, grad_one)
        gain_terms.append(gain_term)
        input_grads[h] = (grad_middle[h] + grad_resid).astype(BF)
    input_grad = joined(input_grads[0], swap(input_grads[1], "seg", 1))
    outputs = joined(result_live[0], swap(result_live[1], "seg", 1))
    gains = jnp.stack([gain_terms[0] + gain_terms[1], gain_two_terms[0] + gain_two_terms[1]])
    gains = sum_all(gains, ("fsdp", "tp", "seg"))
    gain_one_grad, gain_two_grad = lax.dynamic_slice_in_dim(gains, fsdp * depth, depth, axis=1)
    return (outputs, input_grad, gain_one_grad, grad_qkv, grad_out, gain_two_grad, grad_gu, grad_down)


def solution(mesh):
    fsdp, tp = mesh.devices.shape
    inner = Mesh(mesh.devices.reshape(fsdp, SEG, tp // SEG), ("fsdp", "seg", "tp"))
    act = P(None, "fsdp", ("seg", "tp"), None)
    col = P("fsdp", None, ("seg", "tp"))
    row = P(("seg", "tp"), "fsdp")
    return jax.shard_map(
        layer,
        mesh=inner,
        in_specs=(act, act, P(), P("fsdp"), col, row, P("fsdp"), col, row),
        out_specs=(act, act, P("fsdp"), col, row, P("fsdp"), col, row),
        check_vma=False,
    )
```

```python
import functools
import math

import jax
import jax.numpy as jnp
from jax import lax
from jax.experimental import pallas as pl
from jax.experimental.pallas import tpu as pltpu
from jax.sharding import Mesh
from jax.sharding import PartitionSpec as P


HD = 64
NORM_EPS = 1e-05
ROPE_THETA = 130000.0
BLK = 256
SEG = 2
BF = jnp.bfloat16
F32 = jnp.float32
NEG = -1e30
SCALE = 1.0 / math.sqrt(HD)
LOG2E = math.log2(math.e)
VMEM_BYTES = 60 * 1024 * 1024


OWN, OTHER = 0, 1


def swap(x, axis, bit):
    size = lax.axis_size(axis)
    return lax.ppermute(x, axis, [(i, i ^ bit) for i in range(size)])


def gather_slots(x, axis):
    size = lax.axis_size(axis)
    slots = {0: x}
    bit = size // 2
    while bit:
        for k in list(slots):
            slots[k | bit] = swap(slots[k], axis, bit)
        bit //= 2
    return [slots[k] for k in range(size)]


def scatter_slots(parts, axis):
    slots = dict(enumerate(parts))
    bit = 1
    while bit < lax.axis_size(axis):
        for k in [k for k in slots if k & bit]:
            got = swap(slots.pop(k), axis, bit)
            kept = slots[k ^ bit].astype(F32) + got.astype(F32)
            slots[k ^ bit] = kept if bit * 2 == lax.axis_size(axis) else kept.astype(BF)
        bit *= 2
    return slots[0]


def join_kernel(*refs):
    rows = refs[0].shape[0]
    for k, block in enumerate(refs[:-1]):
        refs[-1][k * rows : (k + 1) * rows, :] = block[...]


def join(blocks):
    rows, dim = blocks[0].shape
    cols = dim // 4
    total = rows * len(blocks)
    return pl.pallas_call(
        join_kernel,
        grid=(4,),
        in_specs=[pl.BlockSpec((rows, cols), lambda i: (0, i))] * len(blocks),
        out_specs=pl.BlockSpec((total, cols), lambda i: (0, i)),
        out_shape=jax.ShapeDtypeStruct((total, dim), blocks[0].dtype),
        compiler_params=pltpu.CompilerParams(vmem_limit_bytes=24 * 1024 * 1024),
        cost_estimate=pl.CostEstimate(flops=0, bytes_accessed=4 * total * dim, transcendentals=0),
    )(*blocks)


def gather_rows(local):
    blocks = gather_slots(local, "tp")
    return join([b[h] for h in range(2) for b in blocks])


def scatter_rows(full, rows):
    size = lax.axis_size("tp")
    parts = full.reshape(2, size, rows, full.shape[-1])
    return scatter_slots([parts[:, k] for k in range(size)], "tp")


def scatter_half(half, rows):
    parts = half.reshape(-1, rows, half.shape[-1])
    return scatter_slots([parts[k] for k in range(parts.shape[0])], "tp")


def sum_all(x, axes):
    for axis in axes:
        bit = 1
        while bit < lax.axis_size(axis):
            x = x + swap(x, axis, bit)
            bit *= 2
    return x


def qkv_kernel(x_ref, w_ref, cos_ref, sa_ref, sb_ref, o_ref):
    acc = jnp.dot(x_ref[...], w_ref[...], preferred_element_type=F32)
    cos, sin_a, sin_b = cos_ref[...], sa_ref[...], sb_ref[...]
    for part in range(o_ref.shape[1] // 128):
        lanes = slice(part * 128, part * 128 + 128)
        u = acc[:, lanes]
        if part % 3 < 2:
            u = u * cos + pltpu.roll(u, 96, 1) * sin_a + pltpu.roll(u, 32, 1) * sin_b
        o_ref[:, lanes] = u.astype(BF)


def qkv_project(rows, weight, cos, sin_a, sin_b):
    seq, dim = rows.shape
    cols = weight.shape[1] // 4 * 3
    row_block = min(BLK, seq)
    return pl.pallas_call(
        qkv_kernel,
        grid=(seq // row_block,),
        in_specs=[
            pl.BlockSpec((row_block, dim), lambda i: (i, 0)),
            pl.BlockSpec((dim, cols), lambda i: (0, 0), pipeline_mode=pl.Buffered(1)),
        ]
        + [pl.BlockSpec((row_block, 128), lambda i: (i, 0))] * 3,
        out_specs=pl.BlockSpec((row_block, cols), lambda i: (i, 0)),
        out_shape=jax.ShapeDtypeStruct((seq, cols), BF),
        compiler_params=pltpu.CompilerParams(vmem_limit_bytes=VMEM_BYTES),
        cost_estimate=pl.CostEstimate(
            flops=2 * seq * dim * cols, bytes_accessed=2 * (seq * dim + dim * cols + seq * cols), transcendentals=0
        ),
        name="qkv_project",
    )(rows, weight, cos, sin_a, sin_b)


def slot_of(block, group, turn, side):
    return jnp.bitwise_xor(block // group, side) * group + jnp.bitwise_xor(block % group, turn)


def lane_masks(rows):
    lane = lax.broadcasted_iota(jnp.int32, (rows, 128), 1)
    return lane < HD, lane >= HD


def diagonal_mask(block, length):
    key = lax.broadcasted_iota(jnp.int32, (BLK, BLK), 0)
    query = lax.broadcasted_iota(jnp.int32, (BLK, BLK), 1)
    return (key <= query) & (key + block * BLK < length)


def attend_kernel(group, info_ref, qkv_ref, o_ref, lse_ref, vt_ref):
    count = qkv_ref.shape[0] // BLK
    length, turn, side = info_ref[0], info_ref[1], info_ref[2]

    def rows_of(block):
        return pl.ds(pl.multiple_of(slot_of(block, group, turn, side) * BLK, BLK), BLK)

    masks = lane_masks(BLK)
    for i in range(count):

        @pl.when(i * BLK < length)
        def _():
            where_q = rows_of(i)
            vt_ref[i] = qkv_ref[where_q, 256:384].T
            q = qkv_ref[where_q, 0:128]
            outs = []
            for h in range(2):
                qt = jnp.where(masks[h], q, jnp.zeros_like(q)).T
                top = total = acc = None
                step = 2
                first = 0
                while first <= i:
                    blocks = list(range(first, min(first + step, i + 1)))
                    scores = []
                    for b in blocks:
                        s = jnp.dot(qkv_ref[rows_of(b), 128:256], qt, preferred_element_type=F32) * (SCALE * LOG2E)
                        if b == i:
                            s = jnp.where(diagonal_mask(i, length), s, NEG)
                        scores.append(s)
                    new_top = functools.reduce(jnp.maximum, [jnp.max(s, axis=0, keepdims=True) for s in scores])
                    if top is not None:
                        new_top = jnp.maximum(top, new_top)
                        fade = jnp.exp2(top - new_top)
                        total, acc = total * fade, acc * fade
                    for b, s in zip(blocks, scores):
                        p = jnp.exp2(s - new_top)
                        p_sum = jnp.sum(p, axis=0, keepdims=True)
                        mixed = jnp.dot(
                            vt_ref[b, h * HD : h * HD + HD, :], p.astype(BF), preferred_element_type=F32
                        )
                        total = p_sum if total is None else total + p_sum
                        acc = mixed if acc is None else acc + mixed
                    top = new_top
                    first += step
                outs.append(acc / total)
                lse_ref[i, h : h + 1, :] = top + jnp.log2(total)
            o_ref[where_q, :] = jnp.concatenate(outs, axis=0).T.astype(BF)

        @pl.when(i * BLK >= length)
        def _():
            o_ref[rows_of(i), :] = jnp.zeros((BLK, 128), BF)
            lse_ref[i] = jnp.zeros((2, BLK), F32)


def attend(info, qkv, group):
    seq, cols = qkv.shape
    pairs = cols // 384
    count = seq // BLK
    return pl.pallas_call(
        functools.partial(attend_kernel, group),
        grid_spec=pltpu.PrefetchScalarGridSpec(
            num_scalar_prefetch=1,
            grid=(pairs,),
            in_specs=[pl.BlockSpec((seq, 384), lambda p, s: (0, p))],
            out_specs=[
                pl.BlockSpec((seq, 128), lambda p, s: (0, p)),
                pl.BlockSpec((None, count, 2, BLK), lambda p, s: (p, 0, 0, 0)),
            ],
            scratch_shapes=[pltpu.VMEM((count, 128, BLK), BF)],
        ),
        out_shape=[
            jax.ShapeDtypeStruct((seq, pairs * 128), BF),
            jax.ShapeDtypeStruct((pairs, count, 2, BLK), F32),
        ],
        compiler_params=pltpu.CompilerParams(vmem_limit_bytes=VMEM_BYTES),
        cost_estimate=pl.CostEstimate(
            flops=pairs * 2 * seq * seq * 2 * 256, bytes_accessed=2 * seq * pairs * 512, transcendentals=pairs * seq * seq
        ),
        name="attend",
    )(info, qkv)


def rope_back(w, cos_t, sin_t):
    half = HD // 2
    upper, lower = w[:half], w[half:]
    return jnp.concatenate([upper * cos_t + lower * sin_t, lower * cos_t - upper * sin_t], axis=0)


def attend_back_kernel(
    group, info_ref, qkv_ref, o_ref, do_ref, lse_ref, cos_ref, sin_ref, d_ref, kt_ref, dk_ref, dv_ref
):
    count = qkv_ref.shape[0] // BLK
    length, turn, side = info_ref[0], info_ref[1], info_ref[2]

    def rows_of(block):
        return pl.ds(pl.multiple_of(slot_of(block, group, turn, side) * BLK, BLK), BLK)

    masks = lane_masks(BLK)
    for i in range(count):

        @pl.when(i * BLK < length)
        def _():
            where_q = rows_of(i)
            kt_ref[i] = qkv_ref[where_q, 128:256].T
            q = qkv_ref[where_q, 0:128]
            do = do_ref[where_q, :]
            product = (o_ref[where_q, :].astype(F32) * do.astype(F32)).T
            zero = jnp.zeros_like(q)
            dq_t = []
            for h in range(2):
                q_h = jnp.where(masks[h], q, zero)
                do_h = jnp.where(masks[h], do, zero)
                qt, dot_t = q_h.T, do_h.T
                lse = lse_ref[i, h : h + 1, :]
                delta = jnp.sum(product[h * HD : h * HD + HD], axis=0, keepdims=True)
                dq = None
                for b in range(i + 1):
                    rows_b = rows_of(b)
                    s = jnp.dot(qkv_ref[rows_b, 128:256], qt, preferred_element_type=F32)
                    s = s * (SCALE * LOG2E) - lse
                    if b == i:
                        s = jnp.where(diagonal_mask(i, length), s, NEG)
                    p = jnp.exp2(s)
                    dp = jnp.dot(qkv_ref[rows_b, 256:384], dot_t, preferred_element_type=F32)
                    ds = (p * (dp - delta)).astype(BF)
                    dv = jnp.dot(p.astype(BF), do_h, preferred_element_type=F32)
                    dk = jnp.dot(ds, q_h, preferred_element_type=F32)
                    if b == i and h == 0:
                        dv_ref[b] = dv
                        dk_ref[b] = dk
                    else:
                        dv_ref[b] += dv
                        dk_ref[b] += dk
                    part = jnp.dot(kt_ref[b, h * HD : h * HD + HD, :], ds, preferred_element_type=F32)
                    dq = part if dq is None else dq + part
                dq_t.append(rope_back(dq * SCALE, cos_ref[i], sin_ref[i]))
            d_ref[where_q, 0:128] = jnp.concatenate(dq_t, axis=0).T.astype(BF)

        @pl.when(i * BLK >= length)
        def _():
            d_ref[rows_of(i), :] = jnp.zeros((BLK, 384), BF)

    for i in range(count):

        @pl.when(i * BLK < length)
        def _():
            where_k = rows_of(i)
            dk_t = dk_ref[i].T * SCALE
            parts = [rope_back(dk_t[h * HD : h * HD + HD], cos_ref[i], sin_ref[i]) for h in range(2)]
            d_ref[where_k, 128:256] = jnp.concatenate(parts, axis=0).T.astype(BF)
            d_ref[where_k, 256:384] = dv_ref[i].astype(BF)


def attend_back(info, qkv, mixed, grad_mixed, lse, cos_t, sin_t, group):
    seq, cols = qkv.shape
    pairs = cols // 384
    count = seq // BLK
    return pl.pallas_call(
        functools.partial(attend_back_kernel, group),
        grid_spec=pltpu.PrefetchScalarGridSpec(
            num_scalar_prefetch=1,
            grid=(pairs,),
            in_specs=[
                pl.BlockSpec((seq, 384), lambda p, s: (0, p)),
                pl.BlockSpec((seq, 128), lambda p, s: (0, p)),
                pl.BlockSpec((seq, 128), lambda p, s: (0, p)),
                pl.BlockSpec((None, count, 2, BLK), lambda p, s: (p, 0, 0, 0)),
                pl.BlockSpec((count, HD // 2, BLK), lambda p, s: (0, 0, 0)),
                pl.BlockSpec((count, HD // 2, BLK), lambda p, s: (0, 0, 0)),
            ],
            out_specs=pl.BlockSpec((seq, 384), lambda p, s: (0, p)),
            scratch_shapes=[
                pltpu.VMEM((count, 128, BLK), BF),
                pltpu.VMEM((count, BLK, 128), F32),
                pltpu.VMEM((count, BLK, 128), F32),
            ],
        ),
        out_shape=jax.ShapeDtypeStruct((seq, pairs * 384), BF),
        compiler_params=pltpu.CompilerParams(vmem_limit_bytes=VMEM_BYTES),
        cost_estimate=pl.CostEstimate(
            flops=pairs * 2 * seq * seq * 5 * 256, bytes_accessed=2 * seq * pairs * 1024, transcendentals=pairs * seq * seq
        ),
        name="attend_back",
    )(info, qkv, mixed, grad_mixed, lse, cos_t, sin_t)


def norm_forward(residual, gain_vec):
    factor = lax.rsqrt(jnp.mean(residual * residual, axis=-1, keepdims=True) + NORM_EPS)
    return residual * factor * gain_vec, factor


def norm_backward(residual, factor, gain_vec, grad_in):
    scaled = grad_in * gain_vec
    grad_resid = factor * scaled - residual * factor**3 * jnp.mean(scaled * residual, axis=-1, keepdims=True)
    grad_gain = jnp.sum(grad_in * residual * factor, axis=tuple(range(grad_in.ndim - 1)))
    return grad_resid, grad_gain


def mul(a, b, dims):
    return lax.dot_general(a, b, (dims, ((), ())), preferred_element_type=F32)


NN, NT, TN = ((1,), (0,)), ((1,), (1,)), ((0,), (0,))


def after(value, *anchors):
    return lax.optimization_barrier((value, *anchors))[0]


def layer(inputs, out_grad, lengths, norm1_gain, qkv_weight, out_weight, norm2_gain, gate_up_weight, down_weight):
    rows, _ = inputs.shape[2:]
    group = lax.axis_size("tp")
    seq = SEG * group * rows
    seg, fsdp, me = lax.axis_index("seg"), lax.axis_index("fsdp"), lax.axis_index("tp")
    length = jnp.sum(
        jnp.where(
            (jnp.arange(lengths.shape[0])[:, None] == seg) & (jnp.arange(lengths.shape[1])[None] == fsdp), lengths, 0
        )
    )

    def parted(stacked):
        mine = lax.dynamic_index_in_dim(stacked[:, 0], seg, 0, keepdims=False)
        other = lax.dynamic_index_in_dim(stacked[:, 0], 1 - seg, 0, keepdims=False)
        return mine, other

    def joined(mine, got):
        return jnp.where(seg == 0, jnp.stack([mine, got]), jnp.stack([got, mine]))[:, None]

    def rows_full(shard):
        return lax.all_gather(shard, "fsdp", axis=0, tiled=True)

    def wide(shard):
        return [rows_full(shard), rows_full(swap(shard, "seg", 1))]

    depth = qkv_weight.shape[0]
    head_cols = qkv_weight.shape[2]
    ff = down_weight.shape[0]
    whole_pairs = head_cols % 128 == 0

    def paired(qkv_cols, out_cols):
        count = out_cols.shape[1] // 128
        by_pair = qkv_cols.reshape(depth, 3, count, 128).transpose(0, 2, 1, 3).reshape(depth, count * 384)
        return jnp.concatenate([by_pair, out_cols], axis=1)

    def unpaired(joint):
        count = joint.shape[1] // 512
        by_pair = joint[:, : count * 384].reshape(depth, count, 3, 128).transpose(0, 2, 1, 3)
        return by_pair.reshape(depth, 3, count * 128), joint[:, count * 384 :]

    x_mine, x_other = parted(inputs)
    x_got = swap(x_other, "seg", 1)
    if whole_pairs:
        w_qkvo = wide(paired(qkv_weight, out_weight.T))
    else:
        both = [jnp.stack([w, swap(w, "seg", 1)], axis=-2) for w in (qkv_weight, out_weight.T)]
        w_qkvo = [rows_full(paired(both[0].reshape(depth, 3, -1), both[1].reshape(depth, -1)))]
    gains = lax.all_gather(jnp.stack([norm1_gain, norm2_gain]), "fsdp", axis=0).astype(F32)
    gain_one = gains[:, 0].reshape(-1)
    gain_two = gains[:, 1].reshape(-1)
    w_down = wide(down_weight.T)
    w_gu = wide(gate_up_weight.reshape(depth, 2 * ff))
    cut = w_qkvo[0].shape[1] // 4 * 3
    w_out = jnp.concatenate([w[:, cut:] for w in w_qkvo], axis=1)

    slot = jnp.arange(group)
    position = (
        jnp.bitwise_xor(jnp.arange(SEG), seg)[:, None, None] * (group * rows)
        + jnp.bitwise_xor(slot, me)[None, :, None] * rows
        + jnp.arange(rows)[None, None, :]
    ).reshape(seq)
    inverse = ROPE_THETA ** (-(jnp.arange(HD // 2).astype(F32) * 2.0) / HD)
    angles = position.astype(F32)[:, None] * jnp.tile(inverse, 4)[None, :]
    cos_tab, sin = jnp.cos(angles), jnp.sin(angles)
    first = (jnp.arange(128) % HD < HD // 2)[None, :]
    sin_a = jnp.where(first, -sin, 0.0)
    sin_b = jnp.where(first, 0.0, sin)
    natural = jnp.arange(seq).astype(F32)
    angles_t = inverse[None, :, None] * natural.reshape(seq // BLK, 1, BLK)
    cos_t, sin_t = jnp.cos(angles_t), jnp.sin(angles_t)
    in_kernel = rows == BLK
    none = jnp.int32(0)
    info = jnp.stack([length, me if in_kernel else none, seg if in_kernel else none]).astype(jnp.int32)
    kernel_group = group if in_kernel else seq // BLK // SEG

    def reorder(full):
        if in_kernel:
            return full
        split = full.reshape(SEG, group, rows, full.shape[-1])
        split = jnp.take(split, jnp.bitwise_xor(jnp.arange(SEG), seg), axis=0)
        return jnp.take(split, jnp.bitwise_xor(slot, me), axis=1).reshape(full.shape)

    own_position = (
        jnp.bitwise_xor(jnp.arange(SEG), seg)[:, None, None] * (group * rows)
        + me * rows
        + jnp.arange(rows)[None, :, None]
    )
    live = (own_position < length).astype(F32)

    halves = [x_mine.astype(F32), x_got.astype(F32)]
    blocks, factor_one = [], []
    for h, x in enumerate(halves):
        if h == 1:
            x = halves[1] = after(x_got, blocks[0][0]).astype(F32)
        normed, factor = norm_forward(x, gain_one)
        normed = lax.optimization_barrier(normed.astype(BF))
        blocks.append(gather_slots(normed, "tp"))
        factor_one.append(factor)
    normed_rows = join(blocks[0] + blocks[1])
    qkv, mixed, lse = [], [], []
    for part, weight in enumerate(w_qkvo):
        qkv_rows = qkv_project(normed_rows, weight, cos_tab, sin_a, sin_b)
        qkv.append(reorder(qkv_rows))
        outs = attend(info, qkv[part], kernel_group)
        mixed.append(outs[0])
        lse.append(outs[1])
    mixed_slots = [reorder(m) for m in mixed]
    half = seq // 2
    middle, factor_two, two_blocks = [None, None], [None, None], [None, None]
    for h in range(2):
        rows_in = jnp.concatenate([m[h * half : (h + 1) * half] for m in mixed_slots], axis=1)
        summed = scatter_half(mul(rows_in, w_out, NT).astype(BF), rows)
        if h == 1:
            summed = after(summed, two_blocks[0][0])
        middle[h] = halves[h] + summed
        normed, factor_two[h] = norm_forward(middle[h], gain_two)
        normed = lax.optimization_barrier(normed.astype(BF))
        two_blocks[h] = gather_slots(normed, "tp")
    two_rows = join(two_blocks[0] + two_blocks[1])

    g_mine, g_other = parted(out_grad)
    g_got = swap(g_other, "seg", 1)
    grad_result = jnp.stack([g_mine, g_got]).astype(F32) * live
    grad_rows = gather_rows(grad_result.astype(BF))

    gates, ups, hidden = [], [], []
    for c in range(2):
        gate = mul(two_rows, w_gu[c][:, :ff], NN).astype(BF)
        upward = mul(two_rows, w_gu[c][:, ff:], NN).astype(BF)
        gate32 = gate.astype(F32)
        hid = (gate32 * jax.nn.sigmoid(gate32) * upward.astype(F32)).astype(BF)
        gate, upward, hid = lax.optimization_barrier((gate, upward, hid))
        gates.append(gate)
        ups.append(upward)
        hidden.append(hid)
    product = mul(jnp.concatenate(hidden, axis=1), jnp.concatenate(w_down, axis=1), NT)
    projected = scatter_rows(product.astype(BF), rows)
    grad_parts = []
    for c in range(2):
        grad_hidden = mul(grad_rows, w_down[c], NN)
        gate32, up32 = gates[c].astype(F32), ups[c].astype(F32)
        sig = jax.nn.sigmoid(gate32)
        grad_gate = (grad_hidden * up32 * sig * (1.0 + gate32 * (1.0 - sig))).astype(BF)
        grad_up = (grad_hidden * gate32 * sig).astype(BF)
        grad_parts += [grad_gate, grad_up]

    def reduce_rows(full):
        return lax.psum_scatter(full.astype(BF), "fsdp", scatter_dimension=0, tiled=True)

    def reduce_parts(terms):
        sums = [reduce_rows(t) for t in terms]
        return sums[OWN].astype(F32) + swap(sums[OTHER], "seg", 1).astype(F32)

    grad_down = reduce_parts([mul(grad_rows, hidden[c], TN) for c in range(2)]).T
    copies = lax.optimization_barrier(grad_parts)
    terms = [mul(two_rows, jnp.concatenate(copies[2 * c : 2 * c + 2], axis=1), TN) for c in range(2)]
    grad_gu = reduce_parts(terms)
    grad_gu = grad_gu.reshape(depth, 2, ff)
    grad_middle, gain_two_terms, mid_blocks = [None, None], [], [None, None]
    for h in range(2):
        weights = w_gu if h == 0 else lax.optimization_barrier(w_gu)
        grads = grad_parts if h == 0 else lax.optimization_barrier(grad_parts)
        grads = jnp.concatenate([g[h * half : (h + 1) * half] for g in grads], axis=1)
        product = mul(grads, jnp.concatenate(weights, axis=1), NT)
        grad_two = scatter_half(product.astype(BF), rows)
        if h == 1:
            grad_two = after(grad_two, mid_blocks[0][0])
        grad_resid, gain_term = norm_backward(middle[h], factor_two[h], gain_two, grad_two)
        gain_two_terms.append(gain_term)
        grad_middle[h] = grad_result[h] + grad_resid
        mid_blocks[h] = gather_slots(lax.optimization_barrier(grad_middle[h].astype(BF)), "tp")
    mid_rows = join(mid_blocks[0] + mid_blocks[1])
    projected = after(projected, mid_blocks[1][0])
    result_live = [((middle[h] + projected[h]) * live[h]).astype(BF) for h in range(2)]
    raws, qkvo_terms = {}, {}
    for part in reversed(range(len(w_qkvo))):
        grad_mixed = mul(mid_rows, w_qkvo[part][:, cut:], NN).astype(BF)
        raw = attend_back(
            info, qkv[part], mixed[part], reorder(grad_mixed), lse[part], cos_t, sin_t, kernel_group
        )
        raws[part] = reorder(raw)
        term = mul(normed_rows, raws[part], TN).astype(BF)
        out_term = mul(mid_rows, mixed_slots[part], TN).astype(BF)
        qkvo_terms[part] = jnp.concatenate([term, out_term], axis=1)
    if whole_pairs:
        grad_qkv, grad_out = unpaired(reduce_parts([qkvo_terms[0], qkvo_terms[1]]))
    else:
        part_qkv, part_out = unpaired(reduce_rows(qkvo_terms[0]))
        part_qkv, part_out = part_qkv.reshape(depth, 3, SEG, head_cols), part_out.reshape(depth, SEG, head_cols)
        grad_qkv, grad_out = [
            p[..., 0, :].astype(F32) + swap(p[..., 1, :], "seg", 1).astype(F32) for p in (part_qkv, part_out)
        ]
    grad_out = grad_out.T
    weight = jnp.concatenate([w[:, :cut] for w in w_qkvo], axis=1)
    input_grads, gain_terms = [None, None], []
    for h in (1, 0):
        raw = jnp.concatenate([raws[part][h * half : (h + 1) * half] for part in range(len(w_qkvo))], axis=1)
        product = mul(raw, weight, NT).astype(BF)
        grad_one = scatter_half(product, rows)
        if h == 0:
            grad_one = after(grad_one, input_grads[1])
        grad_resid, gain_term = norm_backward(halves[h], factor_one[h], gain_one, grad_one)
        gain_terms.append(gain_term)
        input_grads[h] = (grad_middle[h] + grad_resid).astype(BF)
    input_grad = joined(input_grads[0], swap(input_grads[1], "seg", 1))
    outputs = joined(result_live[0], swap(result_live[1], "seg", 1))
    gains = jnp.stack([gain_terms[0] + gain_terms[1], gain_two_terms[0] + gain_two_terms[1]])
    gains = sum_all(gains, ("fsdp", "tp", "seg"))
    gain_one_grad, gain_two_grad = lax.dynamic_slice_in_dim(gains, fsdp * depth, depth, axis=1)
    return (outputs, input_grad, gain_one_grad, grad_qkv, grad_out, gain_two_grad, grad_gu, grad_down)


def solution(mesh):
    fsdp, tp = mesh.devices.shape
    inner = Mesh(mesh.devices.reshape(fsdp, SEG, tp // SEG), ("fsdp", "seg", "tp"))
    act = P(None, "fsdp", ("seg", "tp"), None)
    col = P("fsdp", None, ("seg", "tp"))
    row = P(("seg", "tp"), "fsdp")
    return jax.shard_map(
        layer,
        mesh=inner,
        in_specs=(act, act, P(), P("fsdp"), col, row, P("fsdp"), col, row),
        out_specs=(act, act, P("fsdp"), col, row, P("fsdp"), col, row),
        check_vma=False,
    )
```

```python
import functools
import math

import jax
import jax.numpy as jnp
from jax import lax
from jax.experimental import pallas as pl
from jax.experimental.pallas import tpu as pltpu
from jax.sharding import Mesh
from jax.sharding import PartitionSpec as P


HD = 64
NORM_EPS = 1e-05
ROPE_THETA = 130000.0
BLK = 256
KEY_STEP = 4
SEG = 2
BF = jnp.bfloat16
F32 = jnp.float32
NEG = -1e30
SCALE = 1.0 / math.sqrt(HD)
LOG2E = math.log2(math.e)
VMEM_BYTES = 60 * 1024 * 1024


OWN, OTHER = 0, 1


def swap(x, axis, bit):
    size = lax.axis_size(axis)
    return lax.ppermute(x, axis, [(i, i ^ bit) for i in range(size)])


def gather_slots(x, axis):
    size = lax.axis_size(axis)
    slots = {0: x}
    bit = size // 2
    while bit:
        for k in list(slots):
            slots[k | bit] = swap(slots[k], axis, bit)
        bit //= 2
    return [slots[k] for k in range(size)]


def scatter_slots(parts, axis):
    slots = dict(enumerate(parts))
    bit = 1
    while bit < lax.axis_size(axis):
        for k in [k for k in slots if k & bit]:
            got = swap(slots.pop(k), axis, bit)
            kept = slots[k ^ bit].astype(F32) + got.astype(F32)
            slots[k ^ bit] = kept if bit * 2 == lax.axis_size(axis) else kept.astype(BF)
        bit *= 2
    return slots[0]


def join_kernel(*refs):
    rows = refs[0].shape[0]
    for k, block in enumerate(refs[:-1]):
        refs[-1][k * rows : (k + 1) * rows, :] = block[...]


def join(blocks):
    rows, dim = blocks[0].shape
    cols = dim // 4
    total = rows * len(blocks)
    return pl.pallas_call(
        join_kernel,
        grid=(4,),
        in_specs=[pl.BlockSpec((rows, cols), lambda i: (0, i))] * len(blocks),
        out_specs=pl.BlockSpec((total, cols), lambda i: (0, i)),
        out_shape=jax.ShapeDtypeStruct((total, dim), blocks[0].dtype),
        compiler_params=pltpu.CompilerParams(vmem_limit_bytes=24 * 1024 * 1024),
        cost_estimate=pl.CostEstimate(flops=0, bytes_accessed=4 * total * dim, transcendentals=0),
    )(*blocks)


def gather_rows(local):
    blocks = gather_slots(local, "tp")
    return join([b[h] for h in range(2) for b in blocks])


def scatter_rows(full, rows):
    size = lax.axis_size("tp")
    parts = full.reshape(2, size, rows, full.shape[-1])
    return scatter_slots([parts[:, k] for k in range(size)], "tp")


def scatter_half(half, rows):
    parts = half.reshape(-1, rows, half.shape[-1])
    return scatter_slots([parts[k] for k in range(parts.shape[0])], "tp")


def sum_all(x, axes):
    for axis in axes:
        bit = 1
        while bit < lax.axis_size(axis):
            x = x + swap(x, axis, bit)
            bit *= 2
    return x


def qkv_kernel(x_ref, w_ref, cos_ref, sa_ref, sb_ref, o_ref):
    acc = jnp.dot(x_ref[...], w_ref[...], preferred_element_type=F32)
    cos, sin_a, sin_b = cos_ref[...], sa_ref[...], sb_ref[...]
    for part in range(o_ref.shape[1] // 128):
        lanes = slice(part * 128, part * 128 + 128)
        u = acc[:, lanes]
        if part % 3 < 2:
            u = u * cos + pltpu.roll(u, 96, 1) * sin_a + pltpu.roll(u, 32, 1) * sin_b
        o_ref[:, lanes] = u.astype(BF)


def qkv_project(rows, weight, cos, sin_a, sin_b):
    seq, dim = rows.shape
    cols = weight.shape[1] // 4 * 3
    row_block = min(BLK, seq)
    return pl.pallas_call(
        qkv_kernel,
        grid=(seq // row_block,),
        in_specs=[
            pl.BlockSpec((row_block, dim), lambda i: (i, 0)),
            pl.BlockSpec((dim, cols), lambda i: (0, 0), pipeline_mode=pl.Buffered(1)),
        ]
        + [pl.BlockSpec((row_block, 128), lambda i: (i, 0))] * 3,
        out_specs=pl.BlockSpec((row_block, cols), lambda i: (i, 0)),
        out_shape=jax.ShapeDtypeStruct((seq, cols), BF),
        compiler_params=pltpu.CompilerParams(vmem_limit_bytes=VMEM_BYTES),
        cost_estimate=pl.CostEstimate(
            flops=2 * seq * dim * cols, bytes_accessed=2 * (seq * dim + dim * cols + seq * cols), transcendentals=0
        ),
        name="qkv_project",
    )(rows, weight, cos, sin_a, sin_b)


def slot_of(block, group, turn, side):
    return jnp.bitwise_xor(block // group, side) * group + jnp.bitwise_xor(block % group, turn)


def lane_masks(rows):
    lane = lax.broadcasted_iota(jnp.int32, (rows, 128), 1)
    return lane < HD, lane >= HD


def diagonal_mask(block, length):
    key = lax.broadcasted_iota(jnp.int32, (BLK, BLK), 0)
    query = lax.broadcasted_iota(jnp.int32, (BLK, BLK), 1)
    return (key <= query) & (key + block * BLK < length)


def attend_kernel(group, info_ref, qkv_ref, o_ref, lse_ref, vt_ref):
    count = qkv_ref.shape[0] // BLK
    length, turn, side = info_ref[0], info_ref[1], info_ref[2]

    def rows_of(block):
        return pl.ds(pl.multiple_of(slot_of(block, group, turn, side) * BLK, BLK), BLK)

    masks = lane_masks(BLK)
    for i in range(count):

        @pl.when(i * BLK < length)
        def _():
            where_q = rows_of(i)
            vt_ref[i] = qkv_ref[where_q, 256:384].T
            q = qkv_ref[where_q, 0:128]
            q_t = [jnp.where(masks[h], q, jnp.zeros_like(q)).T for h in range(2)]
            state = [None, None]
            for first in range(0, i + 1, KEY_STEP):
                blocks = range(first, min(first + KEY_STEP, i + 1))
                scores = [[], []]
                for h in range(2):
                    for b in blocks:
                        s = jnp.dot(qkv_ref[rows_of(b), 128:256], q_t[h], preferred_element_type=F32) * (SCALE * LOG2E)
                        if b == i:
                            s = jnp.where(diagonal_mask(i, length), s, NEG)
                        scores[h].append(s)
                for h in range(2):
                    top = functools.reduce(jnp.maximum, [jnp.max(s, axis=0, keepdims=True) for s in scores[h]])
                    total = acc = None
                    if state[h] is not None:
                        old_top, total, acc = state[h]
                        top = jnp.maximum(old_top, top)
                        fade = jnp.exp2(old_top - top)
                        total, acc = total * fade, acc * fade
                    for b, s in zip(blocks, scores[h]):
                        p = jnp.exp2(s - top)
                        p_sum = jnp.sum(p, axis=0, keepdims=True)
                        mixed = jnp.dot(vt_ref[b, h * HD : h * HD + HD, :], p.astype(BF), preferred_element_type=F32)
                        total = p_sum if total is None else total + p_sum
                        acc = mixed if acc is None else acc + mixed
                    state[h] = (top, total, acc)
            for h in range(2):
                top, total, _ = state[h]
                lse_ref[i, h : h + 1, :] = top + jnp.log2(total)
            o_ref[where_q, :] = jnp.concatenate([acc / total for _, total, acc in state], axis=0).T.astype(BF)

        @pl.when(i * BLK >= length)
        def _():
            o_ref[rows_of(i), :] = jnp.zeros((BLK, 128), BF)
            lse_ref[i] = jnp.zeros((2, BLK), F32)


def attend(info, qkv, group):
    seq, cols = qkv.shape
    pairs = cols // 384
    count = seq // BLK
    return pl.pallas_call(
        functools.partial(attend_kernel, group),
        grid_spec=pltpu.PrefetchScalarGridSpec(
            num_scalar_prefetch=1,
            grid=(pairs,),
            in_specs=[pl.BlockSpec((seq, 384), lambda p, s: (0, p))],
            out_specs=[
                pl.BlockSpec((seq, 128), lambda p, s: (0, p)),
                pl.BlockSpec((None, count, 2, BLK), lambda p, s: (p, 0, 0, 0)),
            ],
            scratch_shapes=[pltpu.VMEM((count, 128, BLK), BF)],
        ),
        out_shape=[
            jax.ShapeDtypeStruct((seq, pairs * 128), BF),
            jax.ShapeDtypeStruct((pairs, count, 2, BLK), F32),
        ],
        compiler_params=pltpu.CompilerParams(vmem_limit_bytes=VMEM_BYTES),
        cost_estimate=pl.CostEstimate(
            flops=pairs * 2 * seq * seq * 2 * 256, bytes_accessed=2 * seq * pairs * 512, transcendentals=pairs * seq * seq
        ),
        name="attend",
    )(info, qkv)


def rope_back(w, cos_t, sin_t):
    half = HD // 2
    upper, lower = w[:half], w[half:]
    return jnp.concatenate([upper * cos_t + lower * sin_t, lower * cos_t - upper * sin_t], axis=0)


def attend_back_kernel(
    group, info_ref, qkv_ref, o_ref, do_ref, lse_ref, cos_ref, sin_ref, d_ref, kt_ref, dk_ref, dv_ref
):
    count = qkv_ref.shape[0] // BLK
    length, turn, side = info_ref[0], info_ref[1], info_ref[2]

    def rows_of(block):
        return pl.ds(pl.multiple_of(slot_of(block, group, turn, side) * BLK, BLK), BLK)

    masks = lane_masks(BLK)
    for i in range(count):

        @pl.when(i * BLK < length)
        def _():
            where_q = rows_of(i)
            kt_ref[i] = qkv_ref[where_q, 128:256].T
            q = qkv_ref[where_q, 0:128]
            do = do_ref[where_q, :]
            product = (o_ref[where_q, :].astype(F32) * do.astype(F32)).T
            zero = jnp.zeros_like(q)
            q_h = [jnp.where(masks[h], q, zero) for h in range(2)]
            do_h = [jnp.where(masks[h], do, zero) for h in range(2)]
            q_t, do_t = [x.T for x in q_h], [x.T for x in do_h]
            q_both, do_both = jnp.concatenate(q_h, axis=0), jnp.concatenate(do_h, axis=0)
            lse = [lse_ref[i, h : h + 1, :] for h in range(2)]
            delta = [jnp.sum(product[h * HD : h * HD + HD], axis=0, keepdims=True) for h in range(2)]
            dq = [None, None]
            for b in range(i + 1):
                rows_b = rows_of(b)
                probs, ds = [], []
                for h in range(2):
                    s = jnp.dot(qkv_ref[rows_b, 128:256], q_t[h], preferred_element_type=F32)
                    s = s * (SCALE * LOG2E) - lse[h]
                    if b == i:
                        s = jnp.where(diagonal_mask(i, length), s, NEG)
                    p = jnp.exp2(s)
                    dp = jnp.dot(qkv_ref[rows_b, 256:384], do_t[h], preferred_element_type=F32)
                    ds.append((p * (dp - delta[h])).astype(BF))
                    probs.append(p.astype(BF))
                dv = jnp.dot(jnp.concatenate(probs, axis=1), do_both, preferred_element_type=F32)
                dk = jnp.dot(jnp.concatenate(ds, axis=1), q_both, preferred_element_type=F32)
                if b == i:
                    dv_ref[b] = dv
                    dk_ref[b] = dk
                else:
                    dv_ref[b] += dv
                    dk_ref[b] += dk
                for h in range(2):
                    part = jnp.dot(kt_ref[b, h * HD : h * HD + HD, :], ds[h], preferred_element_type=F32)
                    dq[h] = part if dq[h] is None else dq[h] + part
            dq_t = [rope_back(dq[h] * SCALE, cos_ref[i], sin_ref[i]) for h in range(2)]
            d_ref[where_q, 0:128] = jnp.concatenate(dq_t, axis=0).T.astype(BF)

        @pl.when(i * BLK >= length)
        def _():
            d_ref[rows_of(i), :] = jnp.zeros((BLK, 384), BF)

    for i in range(count):

        @pl.when(i * BLK < length)
        def _():
            where_k = rows_of(i)
            dk_t = dk_ref[i].T * SCALE
            parts = [rope_back(dk_t[h * HD : h * HD + HD], cos_ref[i], sin_ref[i]) for h in range(2)]
            d_ref[where_k, 128:256] = jnp.concatenate(parts, axis=0).T.astype(BF)
            d_ref[where_k, 256:384] = dv_ref[i].astype(BF)


def attend_back(info, qkv, mixed, grad_mixed, lse, cos_t, sin_t, group):
    seq, cols = qkv.shape
    pairs = cols // 384
    count = seq // BLK
    return pl.pallas_call(
        functools.partial(attend_back_kernel, group),
        grid_spec=pltpu.PrefetchScalarGridSpec(
            num_scalar_prefetch=1,
            grid=(pairs,),
            in_specs=[
                pl.BlockSpec((seq, 384), lambda p, s: (0, p)),
                pl.BlockSpec((seq, 128), lambda p, s: (0, p)),
                pl.BlockSpec((seq, 128), lambda p, s: (0, p)),
                pl.BlockSpec((None, count, 2, BLK), lambda p, s: (p, 0, 0, 0)),
                pl.BlockSpec((count, HD // 2, BLK), lambda p, s: (0, 0, 0)),
                pl.BlockSpec((count, HD // 2, BLK), lambda p, s: (0, 0, 0)),
            ],
            out_specs=pl.BlockSpec((seq, 384), lambda p, s: (0, p)),
            scratch_shapes=[
                pltpu.VMEM((count, 128, BLK), BF),
                pltpu.VMEM((count, BLK, 128), F32),
                pltpu.VMEM((count, BLK, 128), F32),
            ],
        ),
        out_shape=jax.ShapeDtypeStruct((seq, pairs * 384), BF),
        compiler_params=pltpu.CompilerParams(vmem_limit_bytes=VMEM_BYTES),
        cost_estimate=pl.CostEstimate(
            flops=pairs * 2 * seq * seq * 5 * 256, bytes_accessed=2 * seq * pairs * 1024, transcendentals=pairs * seq * seq
        ),
        name="attend_back",
    )(info, qkv, mixed, grad_mixed, lse, cos_t, sin_t)


def norm_forward(residual, gain_vec):
    factor = lax.rsqrt(jnp.mean(residual * residual, axis=-1, keepdims=True) + NORM_EPS)
    return residual * factor * gain_vec, factor


def norm_backward(residual, factor, gain_vec, grad_in):
    scaled = grad_in * gain_vec
    grad_resid = factor * scaled - residual * factor**3 * jnp.mean(scaled * residual, axis=-1, keepdims=True)
    grad_gain = jnp.sum(grad_in * residual * factor, axis=tuple(range(grad_in.ndim - 1)))
    return grad_resid, grad_gain


def mul(a, b, dims):
    return lax.dot_general(a, b, (dims, ((), ())), preferred_element_type=F32)


NN, NT, TN = ((1,), (0,)), ((1,), (1,)), ((0,), (0,))


def after(value, *anchors):
    return lax.optimization_barrier((value, *anchors))[0]


def layer(inputs, out_grad, lengths, norm1_gain, qkv_weight, out_weight, norm2_gain, gate_up_weight, down_weight):
    rows, _ = inputs.shape[2:]
    group = lax.axis_size("tp")
    seq = SEG * group * rows
    seg, fsdp, me = lax.axis_index("seg"), lax.axis_index("fsdp"), lax.axis_index("tp")
    length = jnp.sum(
        jnp.where(
            (jnp.arange(lengths.shape[0])[:, None] == seg) & (jnp.arange(lengths.shape[1])[None] == fsdp), lengths, 0
        )
    )

    def parted(stacked):
        mine = lax.dynamic_index_in_dim(stacked[:, 0], seg, 0, keepdims=False)
        other = lax.dynamic_index_in_dim(stacked[:, 0], 1 - seg, 0, keepdims=False)
        return mine, other

    def joined(mine, got):
        return jnp.where(seg == 0, jnp.stack([mine, got]), jnp.stack([got, mine]))[:, None]

    def rows_full(shard):
        return lax.all_gather(shard, "fsdp", axis=0, tiled=True)

    def wide(shard):
        return [rows_full(shard), rows_full(swap(shard, "seg", 1))]

    depth = qkv_weight.shape[0]
    head_cols = qkv_weight.shape[2]
    ff = down_weight.shape[0]
    whole_pairs = head_cols % 128 == 0

    def paired(qkv_cols, out_cols):
        count = out_cols.shape[1] // 128
        by_pair = qkv_cols.reshape(depth, 3, count, 128).transpose(0, 2, 1, 3).reshape(depth, count * 384)
        return jnp.concatenate([by_pair, out_cols], axis=1)

    def unpaired(joint):
        count = joint.shape[1] // 512
        by_pair = joint[:, : count * 384].reshape(depth, count, 3, 128).transpose(0, 2, 1, 3)
        return by_pair.reshape(depth, 3, count * 128), joint[:, count * 384 :]

    x_mine, x_other = parted(inputs)
    x_got = swap(x_other, "seg", 1)
    if whole_pairs:
        w_qkvo = wide(paired(qkv_weight, out_weight.T))
    else:
        both = [jnp.stack([w, swap(w, "seg", 1)], axis=-2) for w in (qkv_weight, out_weight.T)]
        w_qkvo = [rows_full(paired(both[0].reshape(depth, 3, -1), both[1].reshape(depth, -1)))]
    gains = lax.all_gather(jnp.stack([norm1_gain, norm2_gain]), "fsdp", axis=0).astype(F32)
    gain_one = gains[:, 0].reshape(-1)
    gain_two = gains[:, 1].reshape(-1)
    w_down = wide(down_weight.T)
    w_gu = wide(gate_up_weight.reshape(depth, 2 * ff))
    cut = w_qkvo[0].shape[1] // 4 * 3
    w_out = jnp.concatenate([w[:, cut:] for w in w_qkvo], axis=1)

    slot = jnp.arange(group)
    position = (
        jnp.bitwise_xor(jnp.arange(SEG), seg)[:, None, None] * (group * rows)
        + jnp.bitwise_xor(slot, me)[None, :, None] * rows
        + jnp.arange(rows)[None, None, :]
    ).reshape(seq)
    inverse = ROPE_THETA ** (-(jnp.arange(HD // 2).astype(F32) * 2.0) / HD)
    angles = position.astype(F32)[:, None] * jnp.tile(inverse, 4)[None, :]
    cos_tab, sin = jnp.cos(angles), jnp.sin(angles)
    first = (jnp.arange(128) % HD < HD // 2)[None, :]
    sin_a = jnp.where(first, -sin, 0.0)
    sin_b = jnp.where(first, 0.0, sin)
    natural = jnp.arange(seq).astype(F32)
    angles_t = inverse[None, :, None] * natural.reshape(seq // BLK, 1, BLK)
    cos_t, sin_t = jnp.cos(angles_t), jnp.sin(angles_t)
    in_kernel = rows == BLK
    none = jnp.int32(0)
    info = jnp.stack([length, me if in_kernel else none, seg if in_kernel else none]).astype(jnp.int32)
    kernel_group = group if in_kernel else seq // BLK // SEG

    def reorder(full):
        if in_kernel:
            return full
        split = full.reshape(SEG, group, rows, full.shape[-1])
        split = jnp.take(split, jnp.bitwise_xor(jnp.arange(SEG), seg), axis=0)
        return jnp.take(split, jnp.bitwise_xor(slot, me), axis=1).reshape(full.shape)

    own_position = (
        jnp.bitwise_xor(jnp.arange(SEG), seg)[:, None, None] * (group * rows)
        + me * rows
        + jnp.arange(rows)[None, :, None]
    )
    live = (own_position < length).astype(F32)

    halves = [x_mine.astype(F32), x_got.astype(F32)]
    blocks, factor_one = [], []
    for h, x in enumerate(halves):
        if h == 1:
            x = halves[1] = after(x_got, blocks[0][0]).astype(F32)
        normed, factor = norm_forward(x, gain_one)
        normed = lax.optimization_barrier(normed.astype(BF))
        blocks.append(gather_slots(normed, "tp"))
        factor_one.append(factor)
    normed_rows = join(blocks[0] + blocks[1])
    qkv, mixed, lse = [], [], []
    for part, weight in enumerate(w_qkvo):
        qkv_rows = qkv_project(normed_rows, weight, cos_tab, sin_a, sin_b)
        qkv.append(reorder(qkv_rows))
        outs = attend(info, qkv[part], kernel_group)
        mixed.append(outs[0])
        lse.append(outs[1])
    mixed_slots = [reorder(m) for m in mixed]
    half = seq // 2
    middle, factor_two, two_blocks = [None, None], [None, None], [None, None]
    for h in range(2):
        rows_in = jnp.concatenate([m[h * half : (h + 1) * half] for m in mixed_slots], axis=1)
        summed = scatter_half(mul(rows_in, w_out, NT).astype(BF), rows)
        if h == 1:
            summed = after(summed, two_blocks[0][0])
        middle[h] = halves[h] + summed
        normed, factor_two[h] = norm_forward(middle[h], gain_two)
        normed = lax.optimization_barrier(normed.astype(BF))
        two_blocks[h] = gather_slots(normed, "tp")
    two_rows = join(two_blocks[0] + two_blocks[1])

    g_mine, g_other = parted(out_grad)
    g_got = swap(g_other, "seg", 1)
    grad_result = jnp.stack([g_mine, g_got]).astype(F32) * live
    grad_rows = gather_rows(grad_result.astype(BF))

    gates, ups, hidden = [], [], []
    for c in range(2):
        gate = mul(two_rows, w_gu[c][:, :ff], NN).astype(BF)
        upward = mul(two_rows, w_gu[c][:, ff:], NN).astype(BF)
        gate32 = gate.astype(F32)
        hid = (gate32 * jax.nn.sigmoid(gate32) * upward.astype(F32)).astype(BF)
        gate, upward, hid = lax.optimization_barrier((gate, upward, hid))
        gates.append(gate)
        ups.append(upward)
        hidden.append(hid)
    product = mul(jnp.concatenate(hidden, axis=1), jnp.concatenate(w_down, axis=1), NT)
    projected = scatter_rows(product.astype(BF), rows)
    grad_parts = []
    for c in range(2):
        grad_hidden = mul(grad_rows, w_down[c], NN)
        gate32, up32 = gates[c].astype(F32), ups[c].astype(F32)
        sig = jax.nn.sigmoid(gate32)
        grad_gate = (grad_hidden * up32 * sig * (1.0 + gate32 * (1.0 - sig))).astype(BF)
        grad_up = (grad_hidden * gate32 * sig).astype(BF)
        grad_parts += [grad_gate, grad_up]

    def reduce_rows(full):
        return lax.psum_scatter(full.astype(BF), "fsdp", scatter_dimension=0, tiled=True)

    def reduce_parts(terms):
        sums = [reduce_rows(t) for t in terms]
        return sums[OWN].astype(F32) + swap(sums[OTHER], "seg", 1).astype(F32)

    grad_down = reduce_parts([mul(grad_rows, hidden[c], TN) for c in range(2)]).T
    copies = lax.optimization_barrier(grad_parts)
    terms = [mul(two_rows, jnp.concatenate(copies[2 * c : 2 * c + 2], axis=1), TN) for c in range(2)]
    grad_gu = reduce_parts(terms)
    grad_gu = grad_gu.reshape(depth, 2, ff)
    grad_middle, gain_two_terms, mid_blocks = [None, None], [], [None, None]
    for h in range(2):
        weights = w_gu if h == 0 else lax.optimization_barrier(w_gu)
        grads = grad_parts if h == 0 else lax.optimization_barrier(grad_parts)
        grads = jnp.concatenate([g[h * half : (h + 1) * half] for g in grads], axis=1)
        product = mul(grads, jnp.concatenate(weights, axis=1), NT)
        grad_two = scatter_half(product.astype(BF), rows)
        if h == 1:
            grad_two = after(grad_two, mid_blocks[0][0])
        grad_resid, gain_term = norm_backward(middle[h], factor_two[h], gain_two, grad_two)
        gain_two_terms.append(gain_term)
        grad_middle[h] = grad_result[h] + grad_resid
        mid_blocks[h] = gather_slots(lax.optimization_barrier(grad_middle[h].astype(BF)), "tp")
    mid_rows = join(mid_blocks[0] + mid_blocks[1])
    projected = after(projected, mid_blocks[1][0])
    result_live = [((middle[h] + projected[h]) * live[h]).astype(BF) for h in range(2)]
    raws, qkvo_terms = {}, {}
    for part in reversed(range(len(w_qkvo))):
        grad_mixed = mul(mid_rows, w_qkvo[part][:, cut:], NN).astype(BF)
        raw = attend_back(
            info, qkv[part], mixed[part], reorder(grad_mixed), lse[part], cos_t, sin_t, kernel_group
        )
        raws[part] = reorder(raw)
        term = mul(normed_rows, raws[part], TN).astype(BF)
        out_term = mul(mid_rows, mixed_slots[part], TN).astype(BF)
        qkvo_terms[part] = jnp.concatenate([term, out_term], axis=1)
    if whole_pairs:
        grad_qkv, grad_out = unpaired(reduce_parts([qkvo_terms[0], qkvo_terms[1]]))
    else:
        part_qkv, part_out = unpaired(reduce_rows(qkvo_terms[0]))
        part_qkv, part_out = part_qkv.reshape(depth, 3, SEG, head_cols), part_out.reshape(depth, SEG, head_cols)
        grad_qkv, grad_out = [
            p[..., 0, :].astype(F32) + swap(p[..., 1, :], "seg", 1).astype(F32) for p in (part_qkv, part_out)
        ]
    grad_out = grad_out.T
    weight = jnp.concatenate([w[:, :cut] for w in w_qkvo], axis=1)
    input_grads, gain_terms = [None, None], []
    for h in (1, 0):
        raw = jnp.concatenate([raws[part][h * half : (h + 1) * half] for part in range(len(w_qkvo))], axis=1)
        product = mul(raw, weight, NT).astype(BF)
        grad_one = scatter_half(product, rows)
        if h == 0:
            grad_one = after(grad_one, input_grads[1])
        grad_resid, gain_term = norm_backward(halves[h], factor_one[h], gain_one, grad_one)
        gain_terms.append(gain_term)
        input_grads[h] = (grad_middle[h] + grad_resid).astype(BF)
    input_grad = joined(input_grads[0], swap(input_grads[1], "seg", 1))
    outputs = joined(result_live[0], swap(result_live[1], "seg", 1))
    gains = jnp.stack([gain_terms[0] + gain_terms[1], gain_two_terms[0] + gain_two_terms[1]])
    gains = sum_all(gains, ("fsdp", "tp", "seg"))
    gain_one_grad, gain_two_grad = lax.dynamic_slice_in_dim(gains, fsdp * depth, depth, axis=1)
    return (outputs, input_grad, gain_one_grad, grad_qkv, grad_out, gain_two_grad, grad_gu, grad_down)


def solution(mesh):
    fsdp, tp = mesh.devices.shape
    inner = Mesh(mesh.devices.reshape(fsdp, SEG, tp // SEG), ("fsdp", "seg", "tp"))
    act = P(None, "fsdp", ("seg", "tp"), None)
    col = P("fsdp", None, ("seg", "tp"))
    row = P(("seg", "tp"), "fsdp")
    return jax.shard_map(
        layer,
        mesh=inner,
        in_specs=(act, act, P(), P("fsdp"), col, row, P("fsdp"), col, row),
        out_specs=(act, act, P("fsdp"), col, row, P("fsdp"), col, row),
        check_vma=False,
    )
```
